32 devices in a mesh: gx: 2 (over x), gy: 4 (over y, core), gz: 4 (over z).
Axes of the slice: x: 2, y: 2, z: 4, core: 2. Of those that a mesh axis runs over, the one named last changes fastest.
Arguments:
- point_xyz: float32 [1536, 3, 128], P(('gx', 'gy', 'gz')), may hold values from 0 to 64, as said below
- point_weight: float32 [1536, 128], P(('gx', 'gy', 'gz')), may hold values from 0.25 to 2
- block_cell: int32 [1536], P(('gx', 'gy', 'gz')), may hold values from 0 to 2047, as said below
- block_count: int32 [1536], P(('gx', 'gy', 'gz')), may hold values from 1 to 128, as said below
- gauss_mean: float32 [2, 16, 64, 3, 32], P('gx', 'gy', 'gz'), may hold values from 0 to 64, as said below
- gauss_opacity: float32 [2, 16, 64, 32], P('gx', 'gy', 'gz'), may hold values from 0.05 to 1
- gauss_count: int32 [2, 16, 64], P('gx', 'gy', 'gz'), may hold values from 8 to 32, as said below
Outputs:
- point_out: float32 [1536, 4, 128], P(('gx', 'gy', 'gz'))
- gauss_grad: float32 [2, 16, 64, 4, 32], P('gx', 'gy', 'gz')
The draws below stay inside these ranges and needn't reach their ends.
Inputs may be any that keep to these rules, and one draw needn't show every extreme that they name: `block_cell`: no two blocks name the same cell. Of the blocks that one device holds, at most 2 lie in the cells of any one brick (a brick is the 1 x 4 x 16 cells of one device of the grid). `block_count`: the valid points of a block are its first ones. `gauss_count`: the used slots of a cell are its first ones. `point_xyz`: every point lies in the cell of its block: each coordinate minus the cell's index lies in [0, 1]. `gauss_mean`: every centre, used or not, lies in its own cell: each coordinate minus the cell's index lies in [0, 1].
All inputs are finite; a program needn't handle non-finite values.
Results may differ from the reference program's by a relative error of at most 0.0003.
Values sent between devices are 32-bit elements; how exact they have to be, the bound alone decides.
No kernel may reach another device: no remote copies, remote signals or barrier semaphores. Data moves between devices by JAX's collectives and lax.ppermute only.
A program may use at most 64 MiB of HBM per device.

```python
import math
import jax
import jax.numpy as jnp
from jax import lax

CX = 1
CY = 4
CZ = 16
NB = 48
GCAP = 32
PTS = 128
MOST = 2
CELLS_DEV = 64
BRICKS = 32
NX = 2
NY = 16
NZ = 64
BLOCKS = 1536


def route_cells(key):
    baseline_units = jax.random.fold_in(key, 7001)
    width_units = NB // MOST
    busy_run_count = max(1, BRICKS // 16)
    busy_units = min(BRICKS, CELLS_DEV // MOST)
    spare_units = BRICKS * width_units - busy_run_count * busy_units
    quiet_run_count = BRICKS - busy_run_count
    balanced_units = spare_units // quiet_run_count
    leftover_runs = spare_units % quiet_run_count
    run_owner = jax.random.permutation(jax.random.fold_in(baseline_units, 1), BRICKS).astype(jnp.int32)
    surplus_unit = (jax.random.permutation(jax.random.fold_in(baseline_units, 2), quiet_run_count) < leftover_runs).astype(jnp.int32)
    units_per_run = jnp.concatenate([jnp.full((busy_run_count,), busy_units, jnp.int32), balanced_units + surplus_unit])
    run_start = jnp.cumsum(units_per_run) - units_per_run
    scores = jax.random.randint(jax.random.fold_in(baseline_units, 3), (BRICKS, NB), 0, 1 << 12) * NB
    scores = scores + jnp.arange(NB, dtype=jnp.int32)[None, :]
    order_in = jnp.argsort(scores, axis=1).astype(jnp.int32)
    source = jnp.arange(BRICKS, dtype=jnp.int32)[:, None]
    unit_index = (order_in // MOST * BRICKS + source).reshape(-1)
    within = (order_in % MOST).reshape(-1)
    run_index = jnp.sum((run_start[None, :] <= unit_index[:, None]).astype(jnp.int32), axis=1) - 1
    arrival = (unit_index - run_start[run_index]) * MOST + within
    brick = run_owner[run_index]
    cell_scores = jax.random.randint(jax.random.fold_in(baseline_units, 4), (BRICKS, CELLS_DEV), 0, 1 << 12) * CELLS_DEV
    cell_scores = cell_scores + jnp.arange(CELLS_DEV, dtype=jnp.int32)[None, :]
    cell_order = jnp.argsort(cell_scores, axis=1).astype(jnp.int32)
    local_cell = cell_order[brick, arrival]
    bricks_y = NY // CY
    bricks_z = NZ // CZ
    brick_x = brick // (bricks_y * bricks_z)
    brick_y = brick // bricks_z % bricks_y
    brick_z = brick % bricks_z
    cell_x = brick_x * CX + local_cell // (CY * CZ)
    cell_y = brick_y * CY + local_cell // CZ % CY
    cell_z = brick_z * CZ + local_cell % CZ
    return ((cell_x * NY + cell_y) * NZ + cell_z).astype(jnp.int32)


def draw_block_cell(key, part):
    return route_cells(key)


def draw_block_count(key, part):
    counts = jax.random.randint(jax.random.fold_in(key, 21), (BLOCKS,), 1, PTS + 1)
    return counts.at[0].set(PTS).astype(jnp.int32)


def draw_gauss_count(key, part):
    counts = jax.random.randint(jax.random.fold_in(key, 31), (NX, NY, NZ), max(1, GCAP // 4), GCAP + 1)
    return counts.at[0, 0, 0].set(GCAP).astype(jnp.int32)


def draw_point_xyz(key, part):
    cells = route_cells(key)
    coords = jnp.stack([cells // (NY * NZ), cells // NZ % NY, cells % NZ], axis=1).astype(jnp.float32)
    noise = jax.random.uniform(jax.random.fold_in(key, 11), (BLOCKS, 3, PTS), jnp.float32)
    return coords[:, :, None] + noise


def draw_gauss_mean(key, part):
    grid = jnp.stack(jnp.meshgrid(jnp.arange(NX), jnp.arange(NY), jnp.arange(NZ), indexing='ij'), axis=-1)
    grid = grid.astype(jnp.float32)
    noise = jax.random.uniform(jax.random.fold_in(key, 41), (NX, NY, NZ, 3, GCAP), jnp.float32)
    return grid[..., :, None] + noise


def levels(stream_key, shape, pieces, least, top_value):
    level, own = 1.0, jax.random.fold_in(stream_key, 6)
    for axis_at, shards_of in pieces:
        draws = jnp.exp(jax.random.uniform(jax.random.fold_in(own, axis_at), (shards_of,), jnp.float32, least / len(pieces), top_value / len(pieces)))
        level = level * jnp.repeat(draws, shape[axis_at] // shards_of).reshape([-1 if axis == axis_at else 1 for axis in range(len(shape))])
    return level


def setup_inputs(seed: int = 0) -> dict:
    seeds = jax.random.split(jax.random.key(seed), 8)
    return {
        "point_xyz": draw_point_xyz(jax.random.fold_in(seeds[7], 71), 0),
        "point_weight": jnp.clip(jnp.exp(math.log(2.0) - 2.0794415 * jax.random.uniform(seeds[1], (BLOCKS, PTS), jnp.float32) ** levels(seeds[1], (BLOCKS, PTS), ((0, 32),), -0.2, 0.2)), 0.25, 2.0),
        "block_cell": draw_block_cell(jax.random.fold_in(seeds[7], 71), 0),
        "block_count": draw_block_count(jax.random.fold_in(seeds[7], 71), 0),
        "gauss_mean": draw_gauss_mean(jax.random.fold_in(seeds[7], 71), 0),
        "gauss_opacity": jnp.clip(jnp.exp(math.log(1.0) - 2.9957323 * jax.random.uniform(seeds[5], (NX, NY, NZ, GCAP), jnp.float32) ** levels(seeds[5], (NX, NY, NZ, GCAP), ((0, 2), (1, 4), (2, 4)), -0.2, 0.2)), 0.05, 1.0),
        "gauss_count": draw_gauss_count(jax.random.fold_in(seeds[7], 71), 0),
    }


kernel_width = 0.05
cutoff_sq = 0.5
floor_term = math.exp(-10.0)


def window(values, step_x, step_y, step_z, extent):
    anchor = jnp.zeros((), jnp.int32)
    corner = (step_x, step_y, step_z) + (anchor,) * (values.ndim - 3)
    return lax.dynamic_slice(values, corner, tuple(extent) + values.shape[3:])


def pair_block(own_items, own_inv, far_items, far_inv, second, with_far, with_density):
    delta_x = own_items[..., 0, :, None] - far_items[..., 0, None, :]
    delta_y = own_items[..., 1, :, None] - far_items[..., 1, None, :]
    delta_z = own_items[..., 2, :, None] - far_items[..., 2, None, :]
    distance = delta_x * delta_x + delta_y * delta_y + delta_z * delta_z
    falloff = jnp.exp(-distance / cutoff_sq)
    kernel = jnp.exp((falloff - 1.0) * (cutoff_sq / kernel_width))
    own_wt = own_items[..., 3, :, None]
    far_wt = far_items[..., 3, None, :]
    if not second:
        own_sum = jnp.sum(kernel * far_wt, axis=-1)
        far_sum = jnp.sum(kernel * own_wt, axis=-2) if with_far else None
        return own_sum, far_sum
    coupling = 2.0 * own_wt * far_wt * kernel * falloff * (own_inv[..., :, None] + far_inv[..., None, :])
    own_grad = jnp.stack([jnp.sum(coupling * delta_x, axis=-1), jnp.sum(coupling * delta_y, axis=-1),
                          jnp.sum(coupling * delta_z, axis=-1)], axis=-2)
    if with_density:
        own_density = jnp.sum(kernel * far_wt * far_inv[..., None, :], axis=-1)
        own_grad = jnp.concatenate([own_grad, own_density[..., None, :]], axis=-2)
    far_out = None
    if with_far:
        far_grad = -jnp.stack([jnp.sum(coupling * delta_x, axis=-2), jnp.sum(coupling * delta_y, axis=-2),
                               jnp.sum(coupling * delta_z, axis=-2)], axis=-2)
        far_density = jnp.sum(kernel * own_wt * own_inv[..., :, None], axis=-2)
        far_out = jnp.concatenate([far_grad, far_density[..., None, :]], axis=-2)
    return own_grad, far_out


def sweep_pairs(own_items, own_inv, far_grid, far_inv, second, with_density):
    extent = own_items.shape[:3]
    own_len = own_items.shape[-1]
    if second:
        own_acc = jnp.zeros(extent + ((4 if with_density else 3), own_len), jnp.float32)
    else:
        own_acc = jnp.zeros(extent + (own_len,), jnp.float32)

    def one_offset(offset, own_total):
        step_x = (offset // 9).astype(jnp.int32)
        step_y = ((offset // 3) % 3).astype(jnp.int32)
        step_z = (offset % 3).astype(jnp.int32)
        far_items = window(far_grid, step_x, step_y, step_z, extent)
        far_part_inv = window(far_inv, step_x, step_y, step_z, extent) if second else None
        own_part, unused = pair_block(own_items, own_inv, far_items, far_part_inv, second, False, with_density)
        return own_total + own_part

    return lax.fori_loop(0, 27, one_offset, own_acc)


def padded(values):
    return jnp.pad(values, ((1, 1), (1, 1), (1, 1)) + ((0, 0),) * (values.ndim - 3))


def planes(own_items, own_inv, far_grid, far_inv, second, with_density):
    def plane_terms(offset):
        own_plane = lax.dynamic_slice_in_dim(own_items, offset, 1, 0)
        far_plane = lax.dynamic_slice_in_dim(far_grid, offset, 3, 0)
        if second:
            inv_plane = lax.dynamic_slice_in_dim(own_inv, offset, 1, 0)
            far_inv_plane = lax.dynamic_slice_in_dim(far_inv, offset, 3, 0)
        else:
            inv_plane = None
            far_inv_plane = None
        result = sweep_pairs(own_plane, inv_plane, far_plane, far_inv_plane, second, with_density)
        return result[0]

    return lax.map(plane_terms, jnp.arange(NX, dtype=jnp.int32))


def reference(point_xyz, point_weight, block_cell, block_count, gauss_mean, gauss_opacity, gauss_count):
    is_valid = jnp.arange(PTS, dtype=jnp.int32)[None, :] < block_count[:, None]
    weights = jnp.where(is_valid, point_weight, 0.0)
    payload = jnp.concatenate([point_xyz, weights[:, None, :]], axis=1)
    points = jnp.zeros((NX * NY * NZ, 4, PTS), jnp.float32).at[block_cell].set(payload)
    points = points.reshape(NX, NY, NZ, 4, PTS)
    present = jnp.arange(GCAP, dtype=jnp.int32) < gauss_count[..., None]
    gaussians = jnp.concatenate([gauss_mean, jnp.where(present, gauss_opacity, 0.0)[..., None, :]], axis=3)
    total_p = floor_term + planes(points, None, padded(gaussians), None, False, False)
    total_g = floor_term + planes(gaussians, None, padded(points), None, False, False)
    inverse_p = 1.0 / total_p
    inverse_g = 1.0 / total_g
    gradient_p = planes(points, inverse_p, padded(gaussians), padded(inverse_g), True, False)
    gradient_g = planes(gaussians, inverse_g, padded(points), padded(inverse_p), True, True)
    loss_p = jnp.where(points[..., 3, :] > 0.0, -kernel_width * jnp.log(total_p), 0.0)
    cell_result = jnp.concatenate([loss_p[..., None, :], gradient_p], axis=3).reshape(NX * NY * NZ, 4, PTS)
    point_out = cell_result[block_cell]
    grad_opacity = jnp.where(present, -kernel_width * jnp.log(total_g) - kernel_width * gradient_g[..., 3, :], 0.0)
    gauss_grad = jnp.concatenate([gradient_g[..., :3, :], grad_opacity[..., None, :]], axis=3)
    return point_out, gauss_grad
```

```python
import functools
import math

import jax
import jax.numpy as jnp
from jax import lax
from jax.experimental import pallas as pl
from jax.experimental.pallas import tpu as pltpu
from jax.sharding import PartitionSpec as P

MOST = 2
AXES = ("gx", "gy", "gz")
LANES = 128
GROUP = 32

kernel_width = 0.05
cutoff_sq = 0.5
sharp = cutoff_sq / kernel_width
log2e = math.log2(math.e)
scale = math.sqrt(log2e / cutoff_sq)
gain = sharp * log2e
shift = math.log2(gain)
grad_unit = 2.0 / (gain * scale)

VMEM = pl.BlockSpec(memory_space=pltpu.VMEM)
SMEM = pl.BlockSpec(memory_space=pltpu.SMEM)


def div_rem(value, size):
    if size & (size - 1) == 0:
        return lax.shift_right_logical(value, size.bit_length() - 1), value & (size - 1)
    return lax.div(value, size), lax.rem(value, size)


def route_kernel(spans, sizes, cell_ref, count_ref, xyz_ref, wt_ref, out_ref, slot_ref, used_ref):
    blocks, _, pts = xyz_ref.shape
    bricks = sizes[0] * sizes[1] * sizes[2]
    lane = lax.broadcasted_iota(jnp.int32, (1, pts), 1)
    out_ref[:, :, : 4 * pts] = jnp.zeros((out_ref.shape[0], 1, 4 * pts), jnp.float32)
    out_ref[:, :, 4 * pts :] = jnp.full((out_ref.shape[0], 1, LANES), -1.0, jnp.float32)

    def clear(i, carry):
        used_ref[i] = 0
        return carry

    lax.fori_loop(0, bricks, clear, 0, unroll=8)

    def one(b, carry):
        rest, along_z = div_rem(cell_ref[b], spans[2] * sizes[2])
        along_x, along_y = div_rem(rest, spans[1] * sizes[1])
        brick_x, in_x = div_rem(along_x, spans[0])
        brick_y, in_y = div_rem(along_y, spans[1])
        brick_z, in_z = div_rem(along_z, spans[2])
        target = (brick_x * sizes[1] + brick_y) * sizes[2] + brick_z
        local = (in_x * spans[1] + in_y) * spans[2] + in_z
        before = used_ref[target]
        used_ref[target] = before + 1
        slot = target * MOST + before
        slot_ref[b] = slot
        count = count_ref[b]
        for f in range(3):
            out_ref[slot, :, f * pts : (f + 1) * pts] = xyz_ref[b, f : f + 1, :]
        out_ref[slot, :, 3 * pts : 4 * pts] = jnp.where(lane < count, wt_ref[pl.ds(b, 1), :], 0.0)
        head = lax.broadcasted_iota(jnp.int32, (1, LANES), 1)
        tag = jnp.where(head == 0, local, count)
        out_ref[slot, :, 4 * pts :] = tag.astype(jnp.float32)
        return carry

    lax.fori_loop(0, blocks, one, 0)


def lane_ids(shape):
    return lax.broadcasted_iota(jnp.int32, shape, len(shape) - 1)


def tile_of(ref, lead, i):
    j = i // 2
    first = ref[lead + (slice(None), pl.ds(j * LANES, LANES))]
    if i % 2 == 0:
        return first
    second = ref[lead + (slice(None), pl.ds((j + 1) * LANES, LANES))]
    return pltpu.roll(jnp.where(lane_ids(first.shape) < 64, second, first), 64, first.ndim - 1)


def untile(parts, chunk):
    total = None
    lane = lane_ids(parts[0].shape)
    for i, low in ((2 * chunk, None), (2 * chunk - 1, True), (2 * chunk + 1, False)):
        if not 0 <= i < len(parts):
            continue
        part = parts[i]
        if low is not None:
            part = pltpu.roll(part, 64, part.ndim - 1)
            part = jnp.where(lane < 64 if low else lane >= 64, part, 0.0)
        total = part if total is None else total + part
    return jnp.zeros_like(parts[0]) if total is None else total


def slot_view(label, spans, rows, planes, tiles):
    in_y, in_z = div_rem(label, spans[2])
    tile, odd = div_rem(in_z, 2)
    lane = lane_ids((1, LANES))
    start = odd * 32
    mask = jnp.where((lane >= start) & (lane < start + 96), 1.0, 0.0)
    index = [(p * rows + in_y + dy) * tiles + tile for p in range(planes) for dy in range(3)]
    return mask, index


def density_kernel(
    spans, planes, in_ref, gauss_ref, origin_ref,
    pt_ref, tile_ref, zg_ref, label_ref, count_ref,
    rows_ref, acc_ref, red_ref,
):
    slots = in_ref.shape[0]
    pts = LANES
    rows = spans[1] + 2
    tiles = spans[2] // 2
    per = LANES // 8
    batches = slots // per
    for s in range(slots):
        head = in_ref[s, :, 4 * pts : 5 * pts]
        whole = head.astype(jnp.int32)
        label_ref[s] = whole[0, 0]
        count_ref[s] = whole[0, 1]
        for f in range(4):
            rows_ref[s, f : f + 1, :] = in_ref[s, :, f * pts : (f + 1) * pts]
        rows_ref[s, 4:8, :] = jnp.ones((4, pts), jnp.float32)
    field = lane_ids((1, LANES)) & 7
    off = jnp.where(
        field == 0, origin_ref[0], jnp.where(field == 1, origin_ref[1], jnp.where(field == 2, origin_ref[2], 0.0))
    )
    mul = jnp.where(field < 3, scale, 1.0)
    for b in range(batches):
        block = rows_ref[b * per : (b + 1) * per].reshape(per * 8, pts)
        pt_ref[b] = (block.T - off) * mul
    part = lax.broadcasted_iota(jnp.int32, (4, 1), 0)
    goff = jnp.where(
        part == 0, origin_ref[0], jnp.where(part == 1, origin_ref[1], jnp.where(part == 2, origin_ref[2], 0.0))
    )
    gmul = jnp.where(part < 3, scale, 1.0)
    for r in range(planes * rows):
        for i in range(tiles):
            tile_ref[r * tiles + i, 0:4, :] = (tile_of(gauss_ref, (r,), i) - goff) * gmul
            tile_ref[r * tiles + i, 4:8, :] = jnp.zeros((4, LANES), jnp.float32)
    acc_ref[...] = jnp.zeros(acc_ref.shape, jnp.float32)

    def one_slot(slot, carry):
        label = label_ref[slot]

        @pl.when(label >= 0)
        def _():
            batch, place = div_rem(slot, per)
            place = place * 8
            mask, index = slot_view(label, spans, rows, planes, tiles)
            alphas = [tile_ref[j, 3:4, :] * mask for j in index]

            def one_group(g, inner):
                at = pl.ds(pl.multiple_of(g * GROUP, GROUP), GROUP)
                raw = pt_ref[batch, at, :]
                view = pltpu.roll(raw, LANES - place, 1)
                x, y, z, w = (view[:, f : f + 1] for f in range(4))
                total = None
                for n, j in enumerate(index):
                    dx = x - tile_ref[j, 0:1, :]
                    dy = y - tile_ref[j, 1:2, :]
                    dz = z - tile_ref[j, 2:3, :]
                    fall = jnp.exp2(shift - (dx * dx + dy * dy + dz * dz))
                    kern = jnp.exp2(fall)
                    term = kern * alphas[n]
                    total = term if total is None else total + term
                    wk = kern * w
                    acc_ref[j] += jnp.sum(wk.reshape(GROUP // 8, 8, LANES), axis=0) * mask
                zp = 1.0 + jnp.sum(total, axis=1, keepdims=True)
                pt_ref[batch, at, :] = jnp.where(lane_ids(raw.shape) == place + 4, zp, raw)
                return inner

            lax.fori_loop(0, (count_ref[slot] + GROUP - 1) // GROUP, one_group, 0)

        return carry

    lax.fori_loop(0, slots, one_slot, 0)
    red_ref[...] = jnp.zeros(red_ref.shape, jnp.float32)
    for r in range(planes * rows):
        for i in range(tiles):
            red_ref[i, r : r + 1, :] = jnp.sum(acc_ref[r * tiles + i], axis=0, keepdims=True)
    parts = [red_ref[i] for i in range(tiles)]
    for c in range(zg_ref.shape[1] // LANES):
        zg_ref[:, c * LANES : (c + 1) * LANES] = untile(parts, c)[: planes * rows]


def gradient_kernel(
    spans, planes, pt_ref, tin_ref, zg_ref, label_ref, count_ref,
    reply_ref, grad_ref,
    tile_ref, acc_ref, out_ref, red_ref,
):
    slots = reply_ref.shape[0]
    rows = spans[1] + 2
    tiles = spans[2] // 2
    per = LANES // 8
    batches = slots // per
    for r in range(planes * rows):
        for i in range(tiles):
            at = r * tiles + i
            tile_ref[at] = tin_ref[at]
    for i in range(tiles):
        inv = 1.0 / (1.0 + tile_of(zg_ref, (), i))
        for r in range(planes * rows):
            at = r * tiles + i
            tile_ref[at, 4:5, :] = tin_ref[at, 3:4, :] * inv[r : r + 1]
    acc_ref[...] = jnp.zeros(acc_ref.shape, jnp.float32)
    out_ref[...] = jnp.zeros(out_ref.shape, jnp.float32)

    def one_slot(slot, carry):
        label = label_ref[slot]

        @pl.when(label >= 0)
        def _():
            batch, place = div_rem(slot, per)
            place = place * 8
            mask, index = slot_view(label, spans, rows, planes, tiles)

            def one_group(g, inner):
                at = pl.ds(pl.multiple_of(g * GROUP, GROUP), GROUP)
                view = pltpu.roll(pt_ref[batch, at, :], LANES - place, 1)
                x, y, z, w, zp = (view[:, f : f + 1] for f in range(5))
                ip = 1.0 / zp
                px = py = pz = None
                for n, j in enumerate(index):
                    dx = x - tile_ref[j, 0:1, :]
                    dy = y - tile_ref[j, 1:2, :]
                    dz = z - tile_ref[j, 2:3, :]
                    fall = jnp.exp2(shift - (dx * dx + dy * dy + dz * dz))
                    wk = jnp.exp2(fall) * w
                    coef = (tile_ref[j, 3:4, :] * mask) * ip + tile_ref[j, 4:5, :] * mask
                    h = wk * fall * coef
                    dx = h * dx
                    dy = h * dy
                    dz = h * dz
                    px = dx if px is None else px + dx
                    py = dy if py is None else py + dy
                    pz = dz if pz is None else pz + dz
                    den = wk * ip
                    for f, v in enumerate((dx, dy, dz)):
                        acc_ref[j, f] += jnp.sum(v.reshape(GROUP // 8, 8, LANES), axis=0)
                    acc_ref[j, 3] += jnp.sum(den.reshape(GROUP // 8, 8, LANES), axis=0) * mask
                val = out_ref[batch, at, :]
                lane = lane_ids(val.shape)
                for f, v in enumerate((px, py, pz)):
                    val = jnp.where(lane == place + 1 + f, jnp.sum(v, axis=1, keepdims=True) * grad_unit, val)
                out_ref[batch, at, :] = val
                return inner

            lax.fori_loop(0, (count_ref[slot] + GROUP - 1) // GROUP, one_group, 0)

        return carry

    lax.fori_loop(0, slots, one_slot, 0)
    for b in range(batches):
        pt = pt_ref[b]
        lane = lane_ids(pt.shape)
        zp = pltpu.roll(pt, LANES - 4, 1)
        w = pltpu.roll(pt, LANES - 3, 1)
        head = (lane & 7) == 0
        ok = head & (w > 0.0)
        zp = jnp.where(ok, zp, 1.0)
        loss = kernel_width * sharp - kernel_width * jnp.log(zp)
        val = jnp.where(head, jnp.where(ok, loss, 0.0), out_ref[b])
        reply_ref[b * per : (b + 1) * per] = val.T.reshape(per, 8, LANES)[:, :4, :]
    for f in range(4):
        red_ref[...] = jnp.zeros(red_ref.shape, jnp.float32)
        for r in range(planes * rows):
            for i in range(tiles):
                red_ref[i, r : r + 1, :] = jnp.sum(acc_ref[r * tiles + i, f], axis=0, keepdims=True)
        parts = [red_ref[i] for i in range(tiles)]
        unit = -grad_unit if f < 3 else 1.0
        for c in range(grad_ref.shape[2] // LANES):
            grad_ref[f, :, c * LANES : (c + 1) * LANES] = untile(parts, c)[: planes * rows] * unit


def pick_kernel(slot_ref, reply_ref, out_ref):
    def one(b, carry):
        out_ref[b] = reply_ref[slot_ref[b]]
        return carry

    lax.fori_loop(0, out_ref.shape[0], one, 0, unroll=4)


def swap(value, axis, odd):
    count = lax.axis_size(axis)
    pairs = []
    for i in range(odd, count - 1, 2):
        pairs += [(i, i + 1), (i + 1, i)]
    if odd and count % 2 == 0 and count > 2:
        pairs += [(0, count - 1), (count - 1, 0)]
    return lax.ppermute(value, axis, pairs)


def trade(low, high, axis):
    count = lax.axis_size(axis)
    here = lax.axis_index(axis)
    even = here % 2 == 0
    first = swap(jnp.where(even, high, low), axis, 0)
    second = swap(jnp.where(even, low, high), axis, 1) if count > 2 else jnp.zeros_like(first)
    from_low = jnp.where(here > 0, jnp.where(even, second, first), 0.0)
    from_high = jnp.where(here < count - 1, jnp.where(even, first, second), 0.0)
    return from_low, from_high


def on_device(
    point_xyz, point_weight, block_cell, block_count, gauss_mean, gauss_opacity, gauss_count
):
    blocks, _, pts = point_xyz.shape
    span_x, span_y, span_z, _, slots = gauss_mean.shape
    spans = (span_x, span_y, span_z)
    sizes = tuple(lax.axis_size(a) for a in AXES)
    if span_x != 1 or slots != 32 or pts != LANES or span_y < 2 or span_z % 4:
        raise ValueError("unsupported brick")
    bricks = sizes[0] * sizes[1] * sizes[2]
    places = bricks * MOST
    room = -(-places // 16) * 16
    f32 = jnp.float32

    outgoing, send_slot = pl.pallas_call(
        functools.partial(route_kernel, spans, sizes),
        out_shape=(
            jax.ShapeDtypeStruct((places, 1, 5 * pts), f32),
            jax.ShapeDtypeStruct((blocks,), jnp.int32),
        ),
        in_specs=[SMEM, SMEM, VMEM, VMEM],
        out_specs=(VMEM, SMEM),
        scratch_shapes=[pltpu.SMEM((bricks,), jnp.int32)],
        name="route",
    )(block_cell, block_count, point_xyz, point_weight)
    incoming = lax.all_to_all(outgoing, AXES, split_axis=0, concat_axis=0, tiled=True)

    present = jnp.arange(slots, dtype=jnp.int32) < gauss_count[..., None]
    own = jnp.concatenate([gauss_mean, jnp.where(present, gauss_opacity, 0.0)[..., None, :]], axis=3)
    own = own[0].transpose(0, 2, 1, 3).reshape(span_y, 4, span_z * slots)
    if sizes[0] == 2:
        stack = jnp.stack([own, swap(own, "gx", 0)])
    else:
        stack = jnp.stack([own, *trade(own, own, "gx")])
    planes = stack.shape[0]
    rows = span_y + 2
    low, high = trade(stack[:, :1], stack[:, -1:], "gy")
    stack = jnp.concatenate([low, stack, high], axis=1).reshape(planes * rows, 4, span_z * slots)
    low, high = trade(stack[..., :slots], stack[..., -slots:], "gz")
    width = (span_z + 2) * slots
    wide = -(-width // LANES) * LANES
    stack = jnp.concatenate(
        [low, stack, high, jnp.zeros((planes * rows, 4, wide - width), f32)], axis=2
    )
    origin = jnp.stack([lax.axis_index(a) * s for a, s in zip(AXES, spans)]).astype(f32)

    tiles = span_z // 2
    count_tiles = planes * rows * tiles
    tall = -(-(planes * rows) // 8) * 8
    points, gtiles, zg_part, label, count = pl.pallas_call(
        functools.partial(density_kernel, spans, planes),
        out_shape=(
            jax.ShapeDtypeStruct((places // 16, LANES, LANES), f32),
            jax.ShapeDtypeStruct((count_tiles, 8, LANES), f32),
            jax.ShapeDtypeStruct((planes * rows, wide), f32),
            jax.ShapeDtypeStruct((places,), jnp.int32),
            jax.ShapeDtypeStruct((places,), jnp.int32),
        ),
        in_specs=[VMEM, VMEM, SMEM],
        out_specs=(VMEM, VMEM, VMEM, SMEM, SMEM),
        scratch_shapes=[
            pltpu.VMEM((places, 8, LANES), f32),
            pltpu.VMEM((count_tiles, 8, LANES), f32),
            pltpu.VMEM((tiles, tall, LANES), f32),
        ],
        name="density",
    )(incoming, stack, origin)

    part = zg_part.reshape(planes, rows, wide)
    if sizes[0] == 2:
        part = part + swap(part[::-1], "gx", 0)
    else:
        low, high = trade(part[1], part[2], "gx")
        whole = part[0] + low + high
        part = jnp.stack([whole, *trade(whole, whole, "gx")])
    low, high = trade(part[:, :2], part[:, -2:], "gy")
    part = jnp.concatenate([part[:, :2] + low, part[:, 2:-2], part[:, -2:] + high], axis=1)
    edge = 2 * slots
    low, high = trade(part[..., :edge], part[..., width - edge : width], "gz")
    part = jnp.concatenate(
        [
            part[..., :edge] + low,
            part[..., edge : width - edge],
            part[..., width - edge : width] + high,
            jnp.zeros((planes, rows, wide - width), f32),
        ],
        axis=2,
    )
    zg_sum = part.reshape(planes * rows, wide)

    reply, grad_part = pl.pallas_call(
        functools.partial(gradient_kernel, spans, planes),
        out_shape=(
            jax.ShapeDtypeStruct((places, 4, LANES), f32),
            jax.ShapeDtypeStruct((4, planes * rows, wide), f32),
        ),
        in_specs=[VMEM, VMEM, VMEM, SMEM, SMEM],
        out_specs=(VMEM, VMEM),
        scratch_shapes=[
            pltpu.VMEM((count_tiles, 8, LANES), f32),
            pltpu.VMEM((count_tiles, 4, 8, LANES), f32),
            pltpu.VMEM((places // 16, LANES, LANES), f32),
            pltpu.VMEM((tiles, tall, LANES), f32),
        ],
        name="gradient",
    )(points, gtiles, zg_sum, label, count)

    answer = lax.all_to_all(reply, AXES, split_axis=0, concat_axis=0, tiled=True)
    point_out = pl.pallas_call(
        pick_kernel,
        out_shape=jax.ShapeDtypeStruct((blocks, 4, pts), f32),
        in_specs=[SMEM, VMEM],
        out_specs=VMEM,
        name="pick",
    )(send_slot, answer)

    grad = grad_part.reshape(4, planes, rows, wide)
    if sizes[0] == 2:
        grad = grad[:, 0] + swap(grad[:, 1], "gx", 0)
    else:
        low, high = trade(grad[:, 1], grad[:, 2], "gx")
        grad = grad[:, 0] + low + high
    low, high = trade(grad[:, :1], grad[:, -1:], "gy")
    grad = jnp.concatenate(
        [grad[:, 1:2] + low, grad[:, 2:-2], grad[:, -2:-1] + high], axis=1
    )
    low, high = trade(grad[..., :slots], grad[..., width - slots : width], "gz")
    grad = jnp.concatenate(
        [
            grad[..., slots : 2 * slots] + low,
            grad[..., 2 * slots : width - 2 * slots],
            grad[..., width - 2 * slots : width - slots] + high,
        ],
        axis=2,
    )
    grad = grad.reshape(4, span_y, span_z, slots).transpose(1, 2, 0, 3)[None]
    total_g = 1.0 + part[0, 1:-1, slots : width - slots].reshape(1, span_y, span_z, slots)
    opacity = jnp.where(
        present,
        kernel_width * sharp - kernel_width * jnp.log(total_g) - kernel_width * grad[..., 3, :],
        0.0,
    )
    gauss_grad = jnp.concatenate([grad[..., :3, :], opacity[..., None, :]], axis=3)
    return point_out, gauss_grad


def solution(mesh):
    return jax.shard_map(
        on_device,
        mesh=mesh,
        in_specs=(
            P(AXES, None, None),
            P(AXES, None),
            P(AXES),
            P(AXES),
            P("gx", "gy", "gz", None, None),
            P("gx", "gy", "gz", None),
            P("gx", "gy", "gz"),
        ),
        out_specs=(P(AXES, None, None), P("gx", "gy", "gz", None, None)),
        check_vma=False,
    )
```

```python
import functools
import math

import jax
import jax.numpy as jnp
from jax import lax
from jax.experimental import pallas as pl
from jax.experimental.pallas import tpu as pltpu
from jax.sharding import PartitionSpec as P

MOST = 2
AXES = ("gx", "gy", "gz")
LANES = 128
SLOTS = 32

kernel_width = 0.05
cutoff_sq = 0.5
sharp = cutoff_sq / kernel_width
log2e = math.log2(math.e)
scale = math.sqrt(log2e / cutoff_sq)
gain = sharp * log2e
shift = math.log2(gain)
grad_unit = 2.0 / (gain * scale)

VMEM = pl.BlockSpec(memory_space=pltpu.VMEM)
SMEM = pl.BlockSpec(memory_space=pltpu.SMEM)


def div_rem(value, size):
    if size & (size - 1) == 0:
        return lax.shift_right_logical(value, size.bit_length() - 1), value & (size - 1)
    return lax.div(value, size), lax.rem(value, size)


def route_kernel(spans, sizes, cell_ref, count_ref, xyz_ref, wt_ref, out_ref, slot_ref, used_ref):
    blocks, _, pts = xyz_ref.shape
    bricks = sizes[0] * sizes[1] * sizes[2]
    lane = lax.broadcasted_iota(jnp.int32, (1, pts), 1)
    out_ref[:, :, : 4 * pts] = jnp.zeros((out_ref.shape[0], 1, 4 * pts), jnp.float32)
    out_ref[:, :, 4 * pts :] = jnp.full((out_ref.shape[0], 1, LANES), -1.0, jnp.float32)

    def clear(i, carry):
        used_ref[i] = 0
        return carry

    lax.fori_loop(0, bricks, clear, 0, unroll=8)

    def one(b, carry):
        rest, along_z = div_rem(cell_ref[b], spans[2] * sizes[2])
        along_x, along_y = div_rem(rest, spans[1] * sizes[1])
        brick_x, in_x = div_rem(along_x, spans[0])
        brick_y, in_y = div_rem(along_y, spans[1])
        brick_z, in_z = div_rem(along_z, spans[2])
        target = (brick_x * sizes[1] + brick_y) * sizes[2] + brick_z
        local = (in_x * spans[1] + in_y) * spans[2] + in_z
        before = used_ref[target]
        used_ref[target] = before + 1
        slot = target * MOST + before
        slot_ref[b] = slot
        count = count_ref[b]
        for f in range(3):
            out_ref[slot, :, f * pts : (f + 1) * pts] = xyz_ref[b, f : f + 1, :]
        out_ref[slot, :, 3 * pts : 4 * pts] = jnp.where(lane < count, wt_ref[pl.ds(b, 1), :], 0.0)
        head = lax.broadcasted_iota(jnp.int32, (1, LANES), 1)
        tag = jnp.where(head == 0, local, count)
        out_ref[slot, :, 4 * pts :] = tag.astype(jnp.float32)
        return carry

    lax.fori_loop(0, blocks, one, 0)


def lane_ids(shape):
    return lax.broadcasted_iota(jnp.int32, shape, len(shape) - 1)


def sub_ids(shape):
    return lax.broadcasted_iota(jnp.int32, shape, len(shape) - 2)


def bases_of(label, spans, rows, planes):
    in_y, in_z = div_rem(label, spans[2])
    cells = spans[2] + 2
    return [
        pl.multiple_of(((p * rows + in_y + dy) * cells + in_z) * SLOTS, SLOTS)
        for p in range(planes)
        for dy in range(3)
    ]


def spread(block, tables, base, height):
    columns = block.T
    for f, table in enumerate(tables):
        for t in range(height // 8):
            at = pl.ds(pl.multiple_of(base + 8 * t, 8), 8)
            table[at, :] = jnp.broadcast_to(columns[8 * t : 8 * t + 8, f : f + 1], (8, LANES))


def gather_sum(acc_ref, base, height):
    lane = lane_ids((8, LANES))
    sub = sub_ids((8, LANES))
    total = None
    for t in range(height // 8):
        at = pl.ds(pl.multiple_of(base + 8 * t, 8), 8)
        part = jnp.sum(acc_ref[at, :], axis=1, keepdims=True)
        part = jnp.where(lane == sub + 8 * t, part, 0.0)
        total = part if total is None else total + part
    return jnp.sum(total, axis=0, keepdims=True)


def fold8(value):
    return jnp.sum(value.reshape(value.shape[0] // 8, 8, value.shape[1]), axis=0)


def density_kernel(
    spans, planes, in_ref, gauss_ref, origin_ref,
    point_ref, zg_ref, label_ref, list_ref, used_ref,
    mx_ref, my_ref, mz_ref, ma_ref, acc_ref, line_ref,
):
    slots = in_ref.shape[0]
    pts = LANES
    rows = spans[1] + 2
    width = (spans[2] + 2) * SLOTS

    part = sub_ids((8, LANES))
    off = jnp.where(
        part == 0, origin_ref[0], jnp.where(part == 1, origin_ref[1], jnp.where(part == 2, origin_ref[2], 0.0))
    )
    mul = jnp.where(part < 3, scale, 1.0)
    for s in range(slots):
        label_ref[s] = in_ref[s, :, 4 * pts :].astype(jnp.int32)[0, 0]
        for f in range(4):
            point_ref[s, f : f + 1, :] = in_ref[s, :, f * pts : (f + 1) * pts]
        point_ref[s, 4:8, :] = jnp.ones((4, pts), jnp.float32)

    def order(s, n):
        list_ref[n] = s
        return n + (label_ref[s] >= 0).astype(jnp.int32)

    used = lax.fori_loop(0, slots, order, 0)
    used_ref[0] = used
    for s in range(slots):
        point_ref[s] = (point_ref[s] - off) * mul

    def table_row(r, carry):
        for c in range(-(-width // LANES)):
            height = min(LANES, width - c * LANES)
            block = jnp.concatenate(
                [gauss_ref[r, :, c * LANES : (c + 1) * LANES], jnp.zeros((4, LANES), jnp.float32)], axis=0
            )
            spread((block - off) * mul, (mx_ref, my_ref, mz_ref, ma_ref), r * width + c * LANES, height)
        return carry

    lax.fori_loop(0, planes * rows, table_row, 0)
    acc_ref[...] = jnp.zeros(acc_ref.shape, jnp.float32)

    def one(i, carry):
        slot = list_ref[i]
        x, y, z, w = (point_ref[slot, f : f + 1, :] for f in range(4))
        total = jnp.zeros((8, LANES), jnp.float32)
        for base in bases_of(label_ref[slot], spans, rows, planes):
            for c in range(3):
                at = pl.ds(pl.multiple_of(base + c * SLOTS, SLOTS), SLOTS)
                dx = x - mx_ref[at, :]
                dy = y - my_ref[at, :]
                dz = z - mz_ref[at, :]
                kern = jnp.exp2(jnp.exp2(shift - (dx * dx + dy * dy + dz * dz)))
                total = total + fold8(kern * ma_ref[at, :])
                acc_ref[at, :] += kern * w
        point_ref[slot, 4:5, :] = 1.0 + jnp.sum(total, axis=0, keepdims=True)
        return carry

    lax.fori_loop(0, used, one, 0)

    def sum_row(r, carry):
        for c in range(-(-width // LANES)):
            height = min(LANES, width - c * LANES)
            line_ref[0, r, :, c * LANES : (c + 1) * LANES] = gather_sum(
                acc_ref, r * width + c * LANES, height
            )
        return carry

    lax.fori_loop(0, planes * rows, sum_row, 0)
    for r in range(planes * rows):
        zg_ref[r : r + 1, :] = line_ref[0, r]


def gradient_kernel(
    spans, planes, point_ref, gauss_ref, zg_ref, origin_ref, label_ref, list_ref, used_ref,
    reply_ref, grad_ref,
    mx_ref, my_ref, mz_ref, ma_ref, mb_ref, ax_ref, ay_ref, az_ref, ad_ref, line_ref,
):
    rows = spans[1] + 2
    width = (spans[2] + 2) * SLOTS
    part = sub_ids((8, LANES))
    off = jnp.where(
        part == 0, origin_ref[0], jnp.where(part == 1, origin_ref[1], jnp.where(part == 2, origin_ref[2], 0.0))
    )
    mul = jnp.where(part < 3, scale, 1.0)

    for r in range(planes * rows):
        line_ref[0, r] = zg_ref[r : r + 1, :]

    def table_row(r, carry):
        for c in range(-(-width // LANES)):
            height = min(LANES, width - c * LANES)
            lanes = slice(c * LANES, (c + 1) * LANES)
            gauss = gauss_ref[r, :, lanes]
            last = gauss[3:4] / (1.0 + line_ref[0, r, :, lanes])
            block = jnp.concatenate([gauss, jnp.broadcast_to(last, (4, LANES))], axis=0)
            spread(
                (block - off) * mul,
                (mx_ref, my_ref, mz_ref, ma_ref, mb_ref),
                r * width + c * LANES,
                height,
            )
        return carry

    lax.fori_loop(0, planes * rows, table_row, 0)
    for ref in (ax_ref, ay_ref, az_ref, ad_ref):
        ref[...] = jnp.zeros(ref.shape, jnp.float32)

    def one(i, carry):
        slot = list_ref[i]
        x, y, z, w, zp = (point_ref[slot, f : f + 1, :] for f in range(5))
        ip = 1.0 / zp
        px = py = pz = jnp.zeros((8, LANES), jnp.float32)
        for base in bases_of(label_ref[slot], spans, rows, planes):
            for c in range(3):
                at = pl.ds(pl.multiple_of(base + c * SLOTS, SLOTS), SLOTS)
                dx = x - mx_ref[at, :]
                dy = y - my_ref[at, :]
                dz = z - mz_ref[at, :]
                fall = jnp.exp2(shift - (dx * dx + dy * dy + dz * dz))
                wk = jnp.exp2(fall) * w
                h = wk * fall * (ma_ref[at, :] * ip + mb_ref[at, :])
                dx = h * dx
                dy = h * dy
                dz = h * dz
                px = px + fold8(dx)
                py = py + fold8(dy)
                pz = pz + fold8(dz)
                ax_ref[at, :] += dx
                ay_ref[at, :] += dy
                az_ref[at, :] += dz
                ad_ref[at, :] += wk * ip
        loss = jnp.where(w > 0.0, kernel_width * sharp - kernel_width * jnp.log(zp), 0.0)
        reply_ref[slot, 0:1, :] = loss
        for f, v in enumerate((px, py, pz)):
            reply_ref[slot, f + 1 : f + 2, :] = jnp.sum(v, axis=0, keepdims=True) * grad_unit
        return carry

    lax.fori_loop(0, used_ref[0], one, 0)

    def sum_row(r, carry):
        for f, ref in enumerate((ax_ref, ay_ref, az_ref, ad_ref)):
            unit = -grad_unit if f < 3 else 1.0
            for c in range(-(-width // LANES)):
                height = min(LANES, width - c * LANES)
                line_ref[f, r, :, c * LANES : (c + 1) * LANES] = (
                    gather_sum(ref, r * width + c * LANES, height) * unit
                )
        return carry

    lax.fori_loop(0, planes * rows, sum_row, 0)
    for f in range(4):
        for r in range(planes * rows):
            grad_ref[f, r : r + 1, :] = line_ref[f, r]


def pick_kernel(slot_ref, reply_ref, out_ref):
    def one(b, carry):
        out_ref[b] = reply_ref[slot_ref[b]]
        return carry

    lax.fori_loop(0, out_ref.shape[0], one, 0, unroll=4)


def swap(value, axis, odd):
    count = lax.axis_size(axis)
    pairs = []
    for i in range(odd, count - 1, 2):
        pairs += [(i, i + 1), (i + 1, i)]
    if odd and count % 2 == 0 and count > 2:
        pairs += [(0, count - 1), (count - 1, 0)]
    return lax.ppermute(value, axis, pairs)


def trade(low, high, axis):
    count = lax.axis_size(axis)
    here = lax.axis_index(axis)
    even = here % 2 == 0
    first = swap(jnp.where(even, high, low), axis, 0)
    second = swap(jnp.where(even, low, high), axis, 1) if count > 2 else jnp.zeros_like(first)
    from_low = jnp.where(here > 0, jnp.where(even, second, first), 0.0)
    from_high = jnp.where(here < count - 1, jnp.where(even, first, second), 0.0)
    return from_low, from_high


def on_device(
    point_xyz, point_weight, block_cell, block_count, gauss_mean, gauss_opacity, gauss_count
):
    blocks, _, pts = point_xyz.shape
    span_x, span_y, span_z, _, slots = gauss_mean.shape
    spans = (span_x, span_y, span_z)
    sizes = tuple(lax.axis_size(a) for a in AXES)
    if span_x != 1 or slots != SLOTS or pts != LANES or span_y < 2 or span_z % 4:
        raise ValueError("unsupported brick")
    bricks = sizes[0] * sizes[1] * sizes[2]
    places = bricks * MOST
    f32 = jnp.float32

    outgoing, send_slot = pl.pallas_call(
        functools.partial(route_kernel, spans, sizes),
        out_shape=(
            jax.ShapeDtypeStruct((places, 1, 5 * pts), f32),
            jax.ShapeDtypeStruct((blocks,), jnp.int32),
        ),
        in_specs=[SMEM, SMEM, VMEM, VMEM],
        out_specs=(VMEM, SMEM),
        scratch_shapes=[pltpu.SMEM((bricks,), jnp.int32)],
        name="route",
    )(block_cell, block_count, point_xyz, point_weight)
    incoming = lax.all_to_all(outgoing, AXES, split_axis=0, concat_axis=0, tiled=True)

    present = jnp.arange(slots, dtype=jnp.int32) < gauss_count[..., None]
    own = jnp.concatenate([gauss_mean, jnp.where(present, gauss_opacity, 0.0)[..., None, :]], axis=3)
    own = own[0].transpose(0, 2, 1, 3).reshape(span_y, 4, span_z * slots)
    if sizes[0] == 2:
        stack = jnp.stack([own, swap(own, "gx", 0)])
    else:
        stack = jnp.stack([own, *trade(own, own, "gx")])
    planes = stack.shape[0]
    rows = span_y + 2
    low, high = trade(stack[:, :1], stack[:, -1:], "gy")
    stack = jnp.concatenate([low, stack, high], axis=1).reshape(planes * rows, 4, span_z * slots)
    low, high = trade(stack[..., :slots], stack[..., -slots:], "gz")
    width = (span_z + 2) * slots
    wide = -(-width // LANES) * LANES
    stack = jnp.concatenate(
        [low, stack, high, jnp.zeros((planes * rows, 4, wide - width), f32)], axis=2
    )
    origin = jnp.stack([lax.axis_index(a) * s for a, s in zip(AXES, spans)]).astype(f32)

    table = pltpu.VMEM((planes * rows * width, LANES), f32)
    points, zg_part, label, order, used = pl.pallas_call(
        functools.partial(density_kernel, spans, planes),
        out_shape=(
            jax.ShapeDtypeStruct((places, 8, LANES), f32),
            jax.ShapeDtypeStruct((planes * rows, wide), f32),
            jax.ShapeDtypeStruct((places,), jnp.int32),
            jax.ShapeDtypeStruct((places + 1,), jnp.int32),
            jax.ShapeDtypeStruct((1,), jnp.int32),
        ),
        in_specs=[VMEM, VMEM, SMEM],
        out_specs=(VMEM, VMEM, SMEM, SMEM, SMEM),
        scratch_shapes=[table] * 5 + [pltpu.VMEM((1, planes * rows, 1, wide), f32)],
        name="density",
    )(incoming, stack, origin)

    part = zg_part.reshape(planes, rows, wide)
    if sizes[0] == 2:
        part = part + swap(part[::-1], "gx", 0)
    else:
        low, high = trade(part[1], part[2], "gx")
        whole = part[0] + low + high
        part = jnp.stack([whole, *trade(whole, whole, "gx")])
    low, high = trade(part[:, :2], part[:, -2:], "gy")
    part = jnp.concatenate([part[:, :2] + low, part[:, 2:-2], part[:, -2:] + high], axis=1)
    edge = 2 * slots
    low, high = trade(part[..., :edge], part[..., width - edge : width], "gz")
    part = jnp.concatenate(
        [
            part[..., :edge] + low,
            part[..., edge : width - edge],
            part[..., width - edge : width] + high,
            jnp.zeros((planes, rows, wide - width), f32),
        ],
        axis=2,
    )
    zg_sum = part.reshape(planes * rows, wide)

    reply, grad_part = pl.pallas_call(
        functools.partial(gradient_kernel, spans, planes),
        out_shape=(
            jax.ShapeDtypeStruct((places, 4, LANES), f32),
            jax.ShapeDtypeStruct((4, planes * rows, wide), f32),
        ),
        in_specs=[VMEM, VMEM, VMEM, SMEM, SMEM, SMEM, SMEM],
        out_specs=(VMEM, VMEM),
        scratch_shapes=[table] * 9 + [pltpu.VMEM((4, planes * rows, 1, wide), f32)],
        name="gradient",
    )(points, stack, zg_sum, origin, label, order, used)

    answer = lax.all_to_all(reply, AXES, split_axis=0, concat_axis=0, tiled=True)
    point_out = pl.pallas_call(
        pick_kernel,
        out_shape=jax.ShapeDtypeStruct((blocks, 4, pts), f32),
        in_specs=[SMEM, VMEM],
        out_specs=VMEM,
        name="pick",
    )(send_slot, answer)

    grad = grad_part.reshape(4, planes, rows, wide)
    if sizes[0] == 2:
        grad = grad[:, 0] + swap(grad[:, 1], "gx", 0)
    else:
        low, high = trade(grad[:, 1], grad[:, 2], "gx")
        grad = grad[:, 0] + low + high
    low, high = trade(grad[:, :1], grad[:, -1:], "gy")
    grad = jnp.concatenate(
        [grad[:, 1:2] + low, grad[:, 2:-2], grad[:, -2:-1] + high], axis=1
    )
    low, high = trade(grad[..., :slots], grad[..., width - slots : width], "gz")
    grad = jnp.concatenate(
        [
            grad[..., slots : 2 * slots] + low,
            grad[..., 2 * slots : width - 2 * slots],
            grad[..., width - 2 * slots : width - slots] + high,
        ],
        axis=2,
    )
    grad = grad.reshape(4, span_y, span_z, slots).transpose(1, 2, 0, 3)[None]
    total_g = 1.0 + part[0, 1:-1, slots : width - slots].reshape(1, span_y, span_z, slots)
    opacity = jnp.where(
        present,
        kernel_width * sharp - kernel_width * jnp.log(total_g) - kernel_width * grad[..., 3, :],
        0.0,
    )
    gauss_grad = jnp.concatenate([grad[..., :3, :], opacity[..., None, :]], axis=3)
    return point_out, gauss_grad


def solution(mesh):
    return jax.shard_map(
        on_device,
        mesh=mesh,
        in_specs=(
            P(AXES, None, None),
            P(AXES, None),
            P(AXES),
            P(AXES),
            P("gx", "gy", "gz", None, None),
            P("gx", "gy", "gz", None),
            P("gx", "gy", "gz"),
        ),
        out_specs=(P(AXES, None, None), P("gx", "gy", "gz", None, None)),
        check_vma=False,
    )
```

```python
import functools
import math

import jax
import jax.numpy as jnp
from jax import lax
from jax.experimental import pallas as pl
from jax.experimental.pallas import tpu as pltpu
from jax.sharding import PartitionSpec as P


MOST = 2
AXES = ("gx", "gy", "gz")
LANES = 128
SLOTS = 32

kernel_width = 0.05
cutoff_sq = 0.5
sharp = cutoff_sq / kernel_width
log2e = math.log2(math.e)
scale = math.sqrt(log2e / cutoff_sq)
gain = sharp * log2e
shift = math.log2(gain)
grad_unit = 2.0 / (gain * scale)

VMEM = pl.BlockSpec(memory_space=pltpu.VMEM)
SMEM = pl.BlockSpec(memory_space=pltpu.SMEM)


def div_rem(value, size):
    if size & (size - 1) == 0:
        return lax.shift_right_logical(value, size.bit_length() - 1), value & (size - 1)
    return lax.div(value, size), lax.rem(value, size)


def route_kernel(spans, sizes, cell_ref, count_ref, xyz_ref, wt_ref, out_ref, slot_ref, used_ref):
    blocks, _, pts = xyz_ref.shape
    bricks = sizes[0] * sizes[1] * sizes[2]
    lane = lax.broadcasted_iota(jnp.int32, (1, pts), 1)
    out_ref[:, :, : 4 * pts] = jnp.zeros((out_ref.shape[0], 1, 4 * pts), jnp.float32)
    out_ref[:, :, 4 * pts :] = jnp.full((out_ref.shape[0], 1, LANES), -1.0, jnp.float32)

    def clear(i, carry):
        used_ref[i] = 0
        return carry

    lax.fori_loop(0, bricks, clear, 0, unroll=8)

    def one(b, carry):
        rest, along_z = div_rem(cell_ref[b], spans[2] * sizes[2])
        along_x, along_y = div_rem(rest, spans[1] * sizes[1])
        brick_x, in_x = div_rem(along_x, spans[0])
        brick_y, in_y = div_rem(along_y, spans[1])
        brick_z, in_z = div_rem(along_z, spans[2])
        target = (brick_x * sizes[1] + brick_y) * sizes[2] + brick_z
        local = (in_x * spans[1] + in_y) * spans[2] + in_z
        before = used_ref[target]
        used_ref[target] = before + 1
        slot = target * MOST + before
        slot_ref[b] = slot
        count = count_ref[b]
        for f in range(3):
            out_ref[slot, :, f * pts : (f + 1) * pts] = xyz_ref[b, f : f + 1, :]
        out_ref[slot, :, 3 * pts : 4 * pts] = jnp.where(lane < count, wt_ref[pl.ds(b, 1), :], 0.0)
        out_ref[slot, :, 4 * pts :] = jnp.full((1, LANES), local, jnp.int32).astype(jnp.float32)
        return carry

    lax.fori_loop(0, blocks, one, 0, unroll=4)


def lane_ids(shape):
    return lax.broadcasted_iota(jnp.int32, shape, len(shape) - 1)


def sub_ids(shape):
    return lax.broadcasted_iota(jnp.int32, shape, len(shape) - 2)


def bases_of(label, spans, rows, planes):
    in_y, in_z = div_rem(label, spans[2])
    cells = spans[2] + 2
    return [
        pl.multiple_of(((p * rows + in_y + dy) * cells + in_z) * SLOTS, SLOTS)
        for p in range(planes)
        for dy in range(3)
    ]


def gather_sum(acc_ref, base, height):
    lane = lane_ids((8, LANES))
    sub = sub_ids((8, LANES))
    total = None
    for t in range(height // 8):
        at = pl.ds(pl.multiple_of(base + 8 * t, 8), 8)
        part = jnp.sum(acc_ref[at, :], axis=1, keepdims=True)
        part = jnp.where(lane == sub + 8 * t, part, 0.0)
        total = part if total is None else total + part
    return jnp.sum(total, axis=0, keepdims=True)


def fold8(value):
    return jnp.sum(value.reshape(value.shape[0] // 8, 8, value.shape[1]), axis=0)


def pieces(value):
    first = value.astype(jnp.bfloat16).astype(jnp.float32)
    rest = value - first
    second = rest.astype(jnp.bfloat16).astype(jnp.float32)
    return first, second, rest - second


def cross_rows(x, y, z, twice):
    rows = []
    split = [pieces(v) for v in (x, y, z)]
    for one in split:
        rows += list(one) if twice else [one[0]] * 3
    for one in split:
        rows += list(one[:2]) if twice else [one[1]] * 2
    for one in split:
        rows += [one[0]] if twice else [one[2]]
    return [v + v for v in rows] if twice else rows


PIECE_ROWS = ((0, 9, 15), (3, 11, 16), (6, 13, 17), (24, 25, 26))


def selector(fields):
    shape = (LANES, LANES * len(fields))
    row = sub_ids(shape)
    lane = lane_ids(shape)
    pick = None
    for n, f in enumerate(fields):
        hit = (row == PIECE_ROWS[f][0]) | (row == PIECE_ROWS[f][1]) | (row == PIECE_ROWS[f][2])
        hit = hit & (lane >= n * LANES) & (lane < (n + 1) * LANES)
        pick = hit if pick is None else pick | hit
    return jnp.where(pick, 1.0, 0.0).astype(jnp.bfloat16)


def product(left, right):
    return jnp.dot(left, right, preferred_element_type=jnp.float32)


def fill(slot, t_ref, label_ref, pair_ref, feat_ref, spans, rows, planes):
    label = label_ref[slot]
    _, in_z = div_rem(label, spans[2])
    near, _ = div_rem(in_z, 4)
    part = pair_ref[pl.ds(pl.multiple_of(slot * 32, 32), 32), :]
    right = jnp.concatenate([part] * 4, axis=0)
    right = jnp.where(lax.shift_right_logical(sub_ids(right.shape), 5) == near, right, 0.0)
    right = right.astype(jnp.bfloat16)
    left = [feat_ref[pl.ds(base, 96), :] for base in bases_of(label, spans, rows, planes)]
    t_ref[...] = product(jnp.concatenate(left, axis=0), right)


def in_turn(used, list_ref, ta_ref, tb_ref, load, use):
    load(list_ref[0], ta_ref)

    def two(i, carry):
        first = list_ref[2 * i]
        second = list_ref[2 * i + 1]
        load(second, tb_ref)
        use(first, ta_ref)
        load(list_ref[2 * i + 2], ta_ref)
        use(second, tb_ref)
        return carry

    lax.fori_loop(0, lax.shift_right_logical(used + 1, 1), two, 0)


def density_kernel(
    spans, planes, in_ref, gauss_ref,
    feat_ref, point_ref, pair_ref, zg_ref, zr_ref, label_ref, list_ref, used_ref,
    raw_ref, fs_ref, ma_ref, acc_ref, line_ref, ta_ref, tb_ref,
):
    slots = in_ref.shape[0]
    pts = LANES
    rows = spans[1] + 2
    width = (spans[2] + 2) * SLOTS
    chunks = -(-width // LANES)
    here = [lax.axis_index(a) * s for a, s in zip(AXES, spans)]
    ref_x = here[0].astype(jnp.float32) + 0.5 * spans[0]
    ref_y = here[1].astype(jnp.float32) + 0.5 * spans[1]
    ref_z = here[2].astype(jnp.float32) + 2.0

    for s in range(slots):
        label_ref[s] = in_ref[s, :, 4 * pts :].astype(jnp.int32)[0, 0]
        for f in range(5):
            raw_ref[f, s : s + 1, :] = in_ref[s, :, f * pts : (f + 1) * pts]
    for f in range(5):
        raw_ref[f, slots : slots + 8, :] = jnp.zeros((8, pts), jnp.float32)
    label_ref[slots] = 0

    def order(s, n):
        list_ref[n] = s
        return n + (label_ref[s] >= 0).astype(jnp.int32)

    used = lax.fori_loop(0, slots, order, 0)
    for n in range(3):
        list_ref[used + n] = slots
    used_ref[0] = used

    for g in range(slots // 8 + 1):
        x, y, z, w, lab = (raw_ref[f, 8 * g : 8 * g + 8, :] for f in range(5))
        lab = jnp.maximum(lab, 0.0)
        in_z = lab - jnp.floor((lab + 0.5) * (1.0 / spans[2])) * spans[2]
        near = jnp.floor((in_z + 0.5) * 0.25) * 4.0
        x = (x - ref_x) * scale
        y = (y - ref_y) * scale
        at_z = (z - (ref_z + near)) * scale
        z = (z - ref_z) * scale
        one = jnp.ones_like(x)
        lines = cross_rows(x, y, at_z, True) + [one] * 3
        lines += list(pieces(0.0 - (x * x + y * y + at_z * at_z)))
        lines += [jnp.zeros_like(x)] * 8
        for k, v in enumerate(lines):
            pair_ref[pl.ds(g * 256 + k, 8, stride=32), :] = v
        for f, v in enumerate((x, y, z, w, one, one, one, one)):
            point_ref[pl.ds(g * 64 + f, 8, stride=8), :] = v

    tall = planes * 8
    fs_ref[...] = jnp.zeros(fs_ref.shape, jnp.float32)
    for c in range(chunks):
        height = min(LANES, width - c * LANES)
        lanes = slice(c * LANES, (c + 1) * LANES)
        for p in range(planes):
            x, y, z, a = (gauss_ref[f, p, :, lanes] for f in range(4))
            x = (x - ref_x) * scale
            y = (y - ref_y) * scale
            plane_sq = x * x + y * y
            for q in range(4):
                at_z = (z - (ref_z + 4.0 * q)) * scale
                lines = cross_rows(x, y, at_z, False)
                lines += list(pieces(shift - (plane_sq + at_z * at_z)))
                lines += [jnp.ones_like(x)] * 3
                if q == 0:
                    lines += list(pieces(a))
                for k, v in enumerate(lines):
                    top = (32 * q + k) * tall + 8 * p
                    fs_ref[top : top + rows, :] = v
        for p in range(planes):
            for r in range(rows):
                block = jnp.concatenate(
                    [fs_ref[pl.ds(8 * t * tall + 8 * p + r, 8, stride=tall), :] for t in range(16)], axis=0
                )
                block = block.T.astype(jnp.bfloat16)
                top = (p * rows + r) * width + c * LANES
                feat_ref[top : top + height, :] = block[:height]
    pick = selector((3,))
    for r in range(planes * rows):
        ma_ref[r * width : (r + 1) * width, :] = product(feat_ref[r * width : (r + 1) * width, :], pick)
    acc_ref[...] = jnp.zeros(acc_ref.shape, jnp.float32)

    def load(slot, t_ref):
        fill(slot, t_ref, label_ref, pair_ref, feat_ref, spans, rows, planes)

    def use(slot, t_ref):
        w = point_ref[pl.ds(pl.multiple_of(slot * 8, 8), 8), :][3:4]
        total = jnp.zeros((8, LANES), jnp.float32)
        for j, base in enumerate(bases_of(label_ref[slot], spans, rows, planes)):
            for c in range(3):
                at = pl.ds(pl.multiple_of(base + c * SLOTS, SLOTS), SLOTS)
                top = j * 96 + c * SLOTS
                kern = jnp.exp2(jnp.exp2(t_ref[top : top + SLOTS, :]))
                total = total + fold8(kern * ma_ref[at, :])
                acc_ref[at, :] += kern * w
        here = pl.ds(pl.multiple_of(slot * 8, 8), 8)
        zp = 1.0 + jnp.sum(total, axis=0, keepdims=True)
        old = point_ref[here, :]
        point_ref[here, :] = jnp.where(sub_ids(old.shape) == 4, zp, old)

    in_turn(used, list_ref, ta_ref, tb_ref, load, use)

    def sum_row(r, carry):
        for c in range(chunks):
            height = min(LANES, width - c * LANES)
            line_ref[0, r, :, c * LANES : (c + 1) * LANES] = gather_sum(
                acc_ref, r * width + c * LANES, height
            )
        return carry

    lax.fori_loop(0, planes * rows, sum_row, 0)
    for p in range(planes):
        for r in range(rows):
            zg_ref[p, r : r + 1, :] = line_ref[0, p * rows + r]
            zr_ref[planes - 1 - p, r : r + 1, :] = line_ref[0, p * rows + r]


def gradient_kernel(
    spans, planes, feat_ref, point_ref, pair_ref, zg_ref, label_ref, list_ref, used_ref,
    reply_ref, grad_ref, other_ref,
    mx_ref, my_ref, mz_ref, ma_ref, mb_ref, ax_ref, ay_ref, az_ref, ad_ref, line_ref, t_ref,
):
    rows = spans[1] + 2
    width = (spans[2] + 2) * SLOTS
    chunks = -(-width // LANES)
    pick = selector((0, 1, 2, 3))
    for r in range(planes * rows):
        at = slice(r * width, (r + 1) * width)
        both = product(feat_ref[at, :], pick)
        for f, ref in enumerate((mx_ref, my_ref, mz_ref, ma_ref)):
            ref[at, :] = both[:, f * LANES : (f + 1) * LANES]
    for c in range(chunks):
        height = min(LANES, width - c * LANES)
        lanes = slice(c * LANES, (c + 1) * LANES)
        block = []
        for p in range(planes):
            block.append(1.0 / (1.0 + zg_ref[p, :, lanes]))
            block.append(jnp.ones((8 - rows, LANES), jnp.float32))
        block = jnp.concatenate(block, axis=0).T
        for p in range(planes):
            for r in range(rows):
                top = (p * rows + r) * width + c * LANES
                at = slice(top, top + height)
                n = p * 8 + r
                mb_ref[at, :] = ma_ref[at, :] * block[:height, n : n + 1]
    for ref in (ax_ref, ay_ref, az_ref, ad_ref):
        ref[...] = jnp.zeros(ref.shape, jnp.float32)

    def use(i, carry):
        slot = list_ref[i]
        x, y, z, w, zp = (point_ref[slot, f : f + 1, :] for f in range(5))
        ip = 1.0 / zp
        px = py = pz = jnp.zeros((8, LANES), jnp.float32)
        for base in bases_of(label_ref[slot], spans, rows, planes):
            for c in range(3):
                at = pl.ds(pl.multiple_of(base + c * SLOTS, SLOTS), SLOTS)
                ex = x - mx_ref[at, :]
                ey = y - my_ref[at, :]
                ez = z - mz_ref[at, :]
                fall = jnp.exp2(shift - (ex * ex + ey * ey + ez * ez))
                wk = jnp.exp2(fall) * w
                h = wk * fall * (ma_ref[at, :] * ip + mb_ref[at, :])
                dx = h * ex
                dy = h * ey
                dz = h * ez
                px = px + fold8(dx)
                py = py + fold8(dy)
                pz = pz + fold8(dz)
                ax_ref[at, :] += dx
                ay_ref[at, :] += dy
                az_ref[at, :] += dz
                ad_ref[at, :] += wk * ip
        loss = jnp.where(w > 0.0, kernel_width * sharp - kernel_width * jnp.log(zp), 0.0)
        reply_ref[slot, 0:1, :] = loss
        for f, v in enumerate((px, py, pz)):
            reply_ref[slot, f + 1 : f + 2, :] = jnp.sum(v, axis=0, keepdims=True) * grad_unit
        return carry

    lax.fori_loop(0, used_ref[0], use, 0)

    def sum_row(r, carry):
        for f, ref in enumerate((ax_ref, ay_ref, az_ref, ad_ref)):
            unit = -grad_unit if f < 3 else 1.0
            for c in range(chunks):
                height = min(LANES, width - c * LANES)
                line_ref[f, r, :, c * LANES : (c + 1) * LANES] = (
                    gather_sum(ref, r * width + c * LANES, height) * unit
                )
        return carry

    lax.fori_loop(0, planes * rows, sum_row, 0)
    for f in range(4):
        for p in range(planes):
            for r in range(rows):
                if p == 0:
                    grad_ref[f, r : r + 1, :] = line_ref[f, r]
                else:
                    other_ref[p - 1, f, r : r + 1, :] = line_ref[f, p * rows + r]


def pick_kernel(slot_ref, reply_ref, out_ref):
    def one(b, carry):
        out_ref[b] = reply_ref[slot_ref[b]]
        return carry

    lax.fori_loop(0, out_ref.shape[0], one, 0, unroll=4)


def swap(value, axis, odd):
    count = lax.axis_size(axis)
    pairs = []
    for i in range(odd, count - 1, 2):
        pairs += [(i, i + 1), (i + 1, i)]
    if odd and count % 2 == 0 and count > 2:
        pairs += [(0, count - 1), (count - 1, 0)]
    return lax.ppermute(value, axis, pairs)


def trade(low, high, axis):
    count = lax.axis_size(axis)
    here = lax.axis_index(axis)
    even = here % 2 == 0
    first = swap(jnp.where(even, high, low), axis, 0)
    second = swap(jnp.where(even, low, high), axis, 1) if count > 2 else jnp.zeros_like(first)
    from_low = jnp.where(here > 0, jnp.where(even, second, first), 0.0)
    from_high = jnp.where(here < count - 1, jnp.where(even, first, second), 0.0)
    return from_low, from_high


def step(
    point_xyz, point_weight, block_cell, block_count, gauss_mean, gauss_opacity, gauss_count
):
    blocks, _, pts = point_xyz.shape
    span_x, span_y, span_z, _, slots = gauss_mean.shape
    spans = (span_x, span_y, span_z)
    sizes = tuple(lax.axis_size(a) for a in AXES)
    if span_x != 1 or slots != SLOTS or pts != LANES or span_y < 2 or span_z % 4:
        raise ValueError("unsupported brick")
    bricks = sizes[0] * sizes[1] * sizes[2]
    places = bricks * MOST
    f32 = jnp.float32

    outgoing, send_slot = pl.pallas_call(
        functools.partial(route_kernel, spans, sizes),
        out_shape=(
            jax.ShapeDtypeStruct((places, 1, 5 * pts), f32),
            jax.ShapeDtypeStruct((blocks,), jnp.int32),
        ),
        in_specs=[SMEM, SMEM, VMEM, VMEM],
        out_specs=(VMEM, SMEM),
        scratch_shapes=[pltpu.SMEM((bricks,), jnp.int32)],
        cost_estimate=pl.CostEstimate(flops=3000000*1000, bytes_accessed=1 << 18, transcendentals=0),
        name="route",
    )(block_cell, block_count, point_xyz, point_weight)
    incoming = lax.all_to_all(outgoing, AXES, split_axis=0, concat_axis=0, tiled=True)

    present = jnp.arange(slots, dtype=jnp.int32) < gauss_count[..., None]
    own = jnp.concatenate([gauss_mean, jnp.where(present, gauss_opacity, 0.0)[..., None, :]], axis=3)
    own = own[0].transpose(2, 0, 1, 3).reshape(4, 1, span_y, span_z * slots)
    if sizes[0] == 2:
        stack = jnp.concatenate([own, swap(own, "gx", 0)], axis=1)
    else:
        stack = jnp.concatenate([own, *trade(own, own, "gx")], axis=1)
    planes = stack.shape[1]
    rows = span_y + 2
    low, high = trade(stack[:, :, :1], stack[:, :, -1:], "gy")
    stack = jnp.concatenate([low, stack, high], axis=2)
    low, high = trade(stack[..., :slots], stack[..., -slots:], "gz")
    width = (span_z + 2) * slots
    wide = -(-width // LANES) * LANES
    stack = jnp.concatenate(
        [low, stack, high, jnp.zeros((4, planes, rows, wide - width), f32)], axis=3
    )

    table = pltpu.VMEM((planes * rows * width, LANES), f32)
    turn = pltpu.VMEM((planes * 3 * 96, LANES), f32)
    feats, points, pairs, part, mirror, label, order, used = pl.pallas_call(
        functools.partial(density_kernel, spans, planes),
        out_shape=(
            jax.ShapeDtypeStruct((planes * rows * width, LANES), jnp.bfloat16),
            jax.ShapeDtypeStruct(((places + 8) * 8, LANES), f32),
            jax.ShapeDtypeStruct(((places + 8) * 32, LANES), f32),
            jax.ShapeDtypeStruct((planes, rows, wide), f32),
            jax.ShapeDtypeStruct((planes, rows, wide), f32),
            jax.ShapeDtypeStruct((places + 1,), jnp.int32),
            jax.ShapeDtypeStruct((places + 3,), jnp.int32),
            jax.ShapeDtypeStruct((1,), jnp.int32),
        ),
        in_specs=[VMEM, VMEM],
        out_specs=(VMEM, VMEM, VMEM, VMEM, VMEM, SMEM, SMEM, SMEM),
        scratch_shapes=[
            pltpu.VMEM((5, places + 8, LANES), f32),
            pltpu.VMEM((LANES * planes * 8, LANES), f32),
            table,
            table,
            pltpu.VMEM((1, planes * rows, 1, wide), f32),
            turn,
            turn,
        ],
        cost_estimate=pl.CostEstimate(flops=15000000*1000, bytes_accessed=1 << 18, transcendentals=0),
        name="density",
    )(incoming, stack)

    if sizes[0] == 2:
        part = part + swap(mirror, "gx", 0)
    else:
        low, high = trade(part[1], part[2], "gx")
        whole = part[0] + low + high
        part = jnp.stack([whole, *trade(whole, whole, "gx")])
    low, high = trade(part[:, :2], part[:, -2:], "gy")
    part = jnp.concatenate([part[:, :2] + low, part[:, 2:-2], part[:, -2:] + high], axis=1)
    edge = 2 * slots
    low, high = trade(part[..., :edge], part[..., width - edge : width], "gz")
    part = jnp.concatenate(
        [
            part[..., :edge] + low,
            part[..., edge : width - edge],
            part[..., width - edge : width] + high,
            jnp.zeros((planes, rows, wide - width), f32),
        ],
        axis=2,
    )
    reply, grad, other = pl.pallas_call(
        functools.partial(gradient_kernel, spans, planes),
        out_shape=(
            jax.ShapeDtypeStruct((places, 4, LANES), f32),
            jax.ShapeDtypeStruct((4, rows, wide), f32),
            jax.ShapeDtypeStruct((planes - 1, 4, rows, wide), f32),
        ),
        in_specs=[VMEM, VMEM, VMEM, VMEM, SMEM, SMEM, SMEM],
        out_specs=(VMEM, VMEM, VMEM),
        scratch_shapes=[table] * 9
        + [pltpu.VMEM((4, planes * rows, 1, wide), f32), pltpu.VMEM((2, planes * 3 * 96, LANES), f32)],
        cost_estimate=pl.CostEstimate(flops=28000000*1000, bytes_accessed=1 << 18, transcendentals=0),
        name="gradient",
    )(feats, points.reshape(places + 8, 8, LANES), pairs, part, label, order, used)

    answer = lax.all_to_all(reply, AXES, split_axis=0, concat_axis=0, tiled=True)
    point_out = pl.pallas_call(
        pick_kernel,
        out_shape=jax.ShapeDtypeStruct((blocks, 4, pts), f32),
        in_specs=[SMEM, VMEM],
        out_specs=VMEM,
        cost_estimate=pl.CostEstimate(flops=2000000*1000, bytes_accessed=1 << 18, transcendentals=0),
        name="pick",
    )(send_slot, answer)

    if sizes[0] == 2:
        grad = grad + swap(other[0], "gx", 0)
    else:
        low, high = trade(other[0], other[1], "gx")
        grad = grad + low + high
    low, high = trade(grad[:, :1], grad[:, -1:], "gy")
    grad = jnp.concatenate(
        [grad[:, 1:2] + low, grad[:, 2:-2], grad[:, -2:-1] + high], axis=1
    )
    low, high = trade(grad[..., :slots], grad[..., width - slots : width], "gz")
    grad = jnp.concatenate(
        [
            grad[..., slots : 2 * slots] + low,
            grad[..., 2 * slots : width - 2 * slots],
            grad[..., width - 2 * slots : width - slots] + high,
        ],
        axis=2,
    )
    grad = grad.reshape(4, span_y, span_z, slots).transpose(1, 2, 0, 3)[None]
    total_g = 1.0 + part[0, 1:-1, slots : width - slots].reshape(1, span_y, span_z, slots)
    opacity = jnp.where(
        present,
        kernel_width * sharp - kernel_width * jnp.log(total_g) - kernel_width * grad[..., 3, :],
        0.0,
    )
    gauss_grad = jnp.concatenate([grad[..., :3, :], opacity[..., None, :]], axis=3)
    return point_out, gauss_grad


def solution(mesh):
    return jax.shard_map(
        step,
        mesh=mesh,
        in_specs=(
            P(AXES, None, None),
            P(AXES, None),
            P(AXES),
            P(AXES),
            P("gx", "gy", "gz", None, None),
            P("gx", "gy", "gz", None),
            P("gx", "gy", "gz"),
        ),
        out_specs=(P(AXES, None, None), P("gx", "gy", "gz", None, None)),
        check_vma=False,
    )
```

```python
import functools
import math

import jax
import jax.numpy as jnp
from jax import lax
from jax.experimental import pallas as pl
from jax.experimental.pallas import tpu as pltpu
from jax.sharding import PartitionSpec as P


MOST = 2
AXES = ("gx", "gy", "gz")
LANES = 128
SLOTS = 32

kernel_width = 0.05
cutoff_sq = 0.5
sharp = cutoff_sq / kernel_width
log2e = math.log2(math.e)
scale = math.sqrt(log2e / cutoff_sq)
gain = sharp * log2e
shift = math.log2(gain)
grad_unit = 2.0 / (gain * scale)

VMEM = pl.BlockSpec(memory_space=pltpu.VMEM)
SMEM = pl.BlockSpec(memory_space=pltpu.SMEM)


def div_rem(value, size):
    if size & (size - 1) == 0:
        return lax.shift_right_logical(value, size.bit_length() - 1), value & (size - 1)
    return lax.div(value, size), lax.rem(value, size)


def route_kernel(spans, sizes, cell_ref, count_ref, xyz_ref, wt_ref, out_ref, slot_ref, used_ref):
    _, blocks, pts = xyz_ref.shape
    bricks = sizes[0] * sizes[1] * sizes[2]
    lane = lax.broadcasted_iota(jnp.int32, (1, pts), 1)
    out_ref[:, :, : 4 * pts] = jnp.zeros((out_ref.shape[0], 1, 4 * pts), jnp.float32)
    out_ref[:, :, 4 * pts :] = jnp.full((out_ref.shape[0], 1, LANES), -1.0, jnp.float32)

    def clear(i, carry):
        used_ref[i] = 0
        return carry

    lax.fori_loop(0, bricks, clear, 0, unroll=8)

    def one(b, carry):
        rest, along_z = div_rem(cell_ref[b], spans[2] * sizes[2])
        along_x, along_y = div_rem(rest, spans[1] * sizes[1])
        brick_x, in_x = div_rem(along_x, spans[0])
        brick_y, in_y = div_rem(along_y, spans[1])
        brick_z, in_z = div_rem(along_z, spans[2])
        target = (brick_x * sizes[1] + brick_y) * sizes[2] + brick_z
        local = (in_x * spans[1] + in_y) * spans[2] + in_z
        before = used_ref[target]
        used_ref[target] = before + 1
        slot = target * MOST + before
        slot_ref[b] = slot
        count = count_ref[b]
        for f in range(3):
            out_ref[slot, :, f * pts : (f + 1) * pts] = xyz_ref[f, pl.ds(b, 1), :]
        out_ref[slot, :, 3 * pts : 4 * pts] = jnp.where(lane < count, wt_ref[pl.ds(b, 1), :], 0.0)
        out_ref[slot, :, 4 * pts :] = jnp.full((1, LANES), local, jnp.int32).astype(jnp.float32)
        return carry

    lax.fori_loop(0, blocks, one, 0, unroll=4)


def route(spans, sizes, point_xyz, point_weight, block_cell, block_count):
    blocks, _, pts = point_xyz.shape
    bricks = sizes[0] * sizes[1] * sizes[2]
    places = bricks * MOST
    f32 = jnp.float32
    return pl.pallas_call(
        functools.partial(route_kernel, spans, sizes),
        out_shape=(
            jax.ShapeDtypeStruct((places, 1, 5 * pts), f32),
            jax.ShapeDtypeStruct((blocks,), jnp.int32),
        ),
        in_specs=[SMEM, SMEM, VMEM, VMEM],
        out_specs=(VMEM, SMEM),
        scratch_shapes=[pltpu.SMEM((bricks,), jnp.int32)],
        cost_estimate=pl.CostEstimate(flops=3000000*1000, bytes_accessed=1 << 18, transcendentals=0),
        name="route",
    )(block_cell, block_count, point_xyz.transpose(1, 0, 2), point_weight)


def lane_ids(shape):
    return lax.broadcasted_iota(jnp.int32, shape, len(shape) - 1)


def sub_ids(shape):
    return lax.broadcasted_iota(jnp.int32, shape, len(shape) - 2)


def bases_of(label, spans, rows, planes):
    in_y, in_z = div_rem(label, spans[2])
    cells = spans[2] + 2
    return [
        pl.multiple_of(((p * rows + in_y + dy) * cells + in_z) * SLOTS, SLOTS)
        for p in range(planes)
        for dy in range(3)
    ]


def gather_sum(acc_ref, base, height):
    lane = lane_ids((8, LANES))
    sub = sub_ids((8, LANES))
    total = None
    for t in range(height // 8):
        at = pl.ds(pl.multiple_of(base + 8 * t, 8), 8)
        part = jnp.sum(acc_ref[at, :], axis=1, keepdims=True)
        part = jnp.where(lane == sub + 8 * t, part, 0.0)
        total = part if total is None else total + part
    return jnp.sum(total, axis=0, keepdims=True)


def clear(refs):
    step = 96

    def some(i, carry):
        at = pl.ds(pl.multiple_of(i * step, 8), step)
        for ref in refs:
            ref[at, :] = jnp.zeros((step, ref.shape[1]), jnp.float32)
        return carry

    lax.fori_loop(0, refs[0].shape[0] // step, some, 0)


def fold8(value):
    return jnp.sum(value.reshape(value.shape[0] // 8, 8, value.shape[1]), axis=0)


def pieces(value):
    first = value.astype(jnp.bfloat16).astype(jnp.float32)
    rest = value - first
    second = rest.astype(jnp.bfloat16).astype(jnp.float32)
    return first, second, rest - second


def cross_rows(x, y, z, twice):
    rows = []
    split = [pieces(v) for v in (x, y, z)]
    for one in split:
        rows += list(one) if twice else [one[0]] * 3
    for one in split:
        rows += list(one[:2]) if twice else [one[1]] * 2
    for one in split:
        rows += [one[0]] if twice else [one[2]]
    return [v + v for v in rows] if twice else rows


PIECE_ROWS = ((0, 9, 15), (3, 11, 16), (6, 13, 17), (24, 25, 26))


def selector(fields):
    shape = (LANES, LANES * len(fields))
    row = sub_ids(shape)
    lane = lane_ids(shape)
    pick = None
    for n, f in enumerate(fields):
        hit = (row == PIECE_ROWS[f][0]) | (row == PIECE_ROWS[f][1]) | (row == PIECE_ROWS[f][2])
        hit = hit & (lane >= n * LANES) & (lane < (n + 1) * LANES)
        pick = hit if pick is None else pick | hit
    return jnp.where(pick, 1.0, 0.0).astype(jnp.bfloat16)


def product(left, right):
    return jnp.dot(left, right, preferred_element_type=jnp.float32)


def fill(slot, t_ref, label_ref, pair_ref, feat_ref, spans, rows, planes):
    label = label_ref[slot]
    _, in_z = div_rem(label, spans[2])
    near, _ = div_rem(in_z, 4)
    part = pair_ref[pl.ds(pl.multiple_of(slot * 32, 32), 32), :]
    right = jnp.concatenate([part] * 4, axis=0)
    right = jnp.where(lax.shift_right_logical(sub_ids(right.shape), 5) == near, right, 0.0)
    right = right.astype(jnp.bfloat16)
    left = [feat_ref[pl.ds(base, 96), :] for base in bases_of(label, spans, rows, planes)]
    t_ref[...] = product(jnp.concatenate(left, axis=0), right)


def in_turn(used, list_ref, ta_ref, tb_ref, load, use):
    load(list_ref[0], ta_ref)

    def two(i, carry):
        first = list_ref[2 * i]
        second = list_ref[2 * i + 1]
        load(second, tb_ref)
        use(first, ta_ref)
        load(list_ref[2 * i + 2], ta_ref)
        use(second, tb_ref)
        return carry

    lax.fori_loop(0, lax.shift_right_logical(used + 1, 1), two, 0)


def density_kernel(
    spans, planes, in_ref, gauss_ref,
    feat_ref, point_ref, zg_ref, zr_ref, label_ref, list_ref, used_ref,
    pair_ref, raw_ref, fs_ref, ma_ref, acc_ref, line_ref, ta_ref, tb_ref,
):
    slots = in_ref.shape[0]
    pts = LANES
    rows = spans[1] + 2
    width = (spans[2] + 2) * SLOTS
    chunks = -(-width // LANES)
    here = [lax.axis_index(a) * s for a, s in zip(AXES, spans)]
    ref_x = here[0].astype(jnp.float32) + 0.5 * spans[0]
    ref_y = here[1].astype(jnp.float32) + 0.5 * spans[1]
    ref_z = here[2].astype(jnp.float32) + 2.0

    for s in range(slots):
        label_ref[s] = in_ref[s, :, 4 * pts :].astype(jnp.int32)[0, 0]
        for f in range(5):
            raw_ref[f, s : s + 1, :] = in_ref[s, :, f * pts : (f + 1) * pts]
    for f in range(5):
        raw_ref[f, slots : slots + 8, :] = jnp.zeros((8, pts), jnp.float32)
    label_ref[slots] = 0

    def order(s, n):
        list_ref[n] = s
        return n + (label_ref[s] >= 0).astype(jnp.int32)

    used = lax.fori_loop(0, slots, order, 0)
    for n in range(3):
        list_ref[used + n] = slots
    used_ref[0] = used

    for g in range(slots // 8 + 1):
        x, y, z, w, lab = (raw_ref[f, 8 * g : 8 * g + 8, :] for f in range(5))
        lab = jnp.maximum(lab, 0.0)
        in_z = lab - jnp.floor((lab + 0.5) * (1.0 / spans[2])) * spans[2]
        near = jnp.floor((in_z + 0.5) * 0.25) * 4.0
        x = (x - ref_x) * scale
        y = (y - ref_y) * scale
        at_z = (z - (ref_z + near)) * scale
        z = (z - ref_z) * scale
        one = jnp.ones_like(x)
        lines = cross_rows(x, y, at_z, True) + [one] * 3
        lines += list(pieces(0.0 - (x * x + y * y + at_z * at_z)))
        lines += [jnp.zeros_like(x)] * 8
        for k, v in enumerate(lines):
            pair_ref[pl.ds(g * 256 + k, 8, stride=32), :] = v
        for f, v in enumerate((x, y, z, w, one, one, one, one)):
            point_ref[pl.ds(g * 64 + f, 8, stride=8), :] = v

    tall = planes * 8
    fs_ref[...] = jnp.zeros(fs_ref.shape, jnp.float32)
    for c in range(chunks):
        height = min(LANES, width - c * LANES)
        lanes = slice(c * LANES, (c + 1) * LANES)
        for p in range(planes):
            x, y, z, a = (gauss_ref[f, p, :, lanes] for f in range(4))
            x = (x - ref_x) * scale
            y = (y - ref_y) * scale
            plane_sq = x * x + y * y
            for q in range(4):
                at_z = (z - (ref_z + 4.0 * q)) * scale
                lines = cross_rows(x, y, at_z, False)
                lines += list(pieces(shift - (plane_sq + at_z * at_z)))
                lines += [jnp.ones_like(x)] * 3
                if q == 0:
                    lines += list(pieces(a))
                for k, v in enumerate(lines):
                    top = (32 * q + k) * tall + 8 * p
                    fs_ref[top : top + rows, :] = v
        for p in range(planes):
            for r in range(rows):
                block = jnp.concatenate(
                    [fs_ref[pl.ds(8 * t * tall + 8 * p + r, 8, stride=tall), :] for t in range(16)], axis=0
                )
                block = block.T.astype(jnp.bfloat16)
                top = (p * rows + r) * width + c * LANES
                feat_ref[top : top + height, :] = block[:height]
    pick = selector((3,))
    for r in range(planes * rows):
        ma_ref[r * width : (r + 1) * width, :] = product(feat_ref[r * width : (r + 1) * width, :], pick)
    clear((acc_ref,))

    def load(slot, t_ref):
        fill(slot, t_ref, label_ref, pair_ref, feat_ref, spans, rows, planes)

    def use(slot, t_ref):
        w = point_ref[pl.ds(pl.multiple_of(slot * 8, 8), 8), :][3:4]
        total = jnp.zeros((8, LANES), jnp.float32)
        for j, base in enumerate(bases_of(label_ref[slot], spans, rows, planes)):
            for c in range(3):
                at = pl.ds(pl.multiple_of(base + c * SLOTS, SLOTS), SLOTS)
                top = j * 96 + c * SLOTS
                kern = jnp.exp2(jnp.exp2(t_ref[top : top + SLOTS, :]))
                total = total + fold8(kern * ma_ref[at, :])
                acc_ref[at, :] += kern * w
        here = pl.ds(pl.multiple_of(slot * 8, 8), 8)
        zp = 1.0 + jnp.sum(total, axis=0, keepdims=True)
        old = point_ref[here, :]
        point_ref[here, :] = jnp.where(sub_ids(old.shape) == 4, zp, old)

    in_turn(used, list_ref, ta_ref, tb_ref, load, use)

    def sum_row(r, carry):
        for c in range(chunks):
            height = min(LANES, width - c * LANES)
            line_ref[0, r, :, c * LANES : (c + 1) * LANES] = gather_sum(
                acc_ref, r * width + c * LANES, height
            )
        return carry

    lax.fori_loop(0, planes * rows, sum_row, 0)
    for p in range(planes):
        for r in range(rows):
            zg_ref[p, r : r + 1, :] = line_ref[0, p * rows + r]
            zr_ref[planes - 1 - p, r : r + 1, :] = line_ref[0, p * rows + r]


def gradient_kernel(
    spans, planes, feat_ref, point_ref, zg_ref, label_ref, list_ref, used_ref,
    reply_ref, grad_ref, other_ref,
    mx_ref, my_ref, mz_ref, ma_ref, mb_ref, ax_ref, ay_ref, az_ref, ad_ref, line_ref, t_ref,
):
    rows = spans[1] + 2
    width = (spans[2] + 2) * SLOTS
    chunks = -(-width // LANES)
    pick = selector((0, 1, 2, 3))
    for r in range(planes * rows):
        at = slice(r * width, (r + 1) * width)
        both = product(feat_ref[at, :], pick)
        for f, ref in enumerate((mx_ref, my_ref, mz_ref, ma_ref)):
            ref[at, :] = both[:, f * LANES : (f + 1) * LANES]
    for c in range(chunks):
        height = min(LANES, width - c * LANES)
        lanes = slice(c * LANES, (c + 1) * LANES)
        block = []
        for p in range(planes):
            block.append(1.0 / (1.0 + zg_ref[p, :, lanes]))
            block.append(jnp.ones((8 - rows, LANES), jnp.float32))
        block = jnp.concatenate(block, axis=0).T
        for p in range(planes):
            for r in range(rows):
                top = (p * rows + r) * width + c * LANES
                at = slice(top, top + height)
                n = p * 8 + r
                mb_ref[at, :] = ma_ref[at, :] * block[:height, n : n + 1]
    clear((ax_ref, ay_ref, az_ref, ad_ref))

    def use(i, carry):
        slot = list_ref[i]
        x, y, z, w, zp = (point_ref[slot, f : f + 1, :] for f in range(5))
        ip = 1.0 / zp
        px = py = pz = jnp.zeros((8, LANES), jnp.float32)
        for base in bases_of(label_ref[slot], spans, rows, planes):
            for c in range(3):
                at = pl.ds(pl.multiple_of(base + c * SLOTS, SLOTS), SLOTS)
                ex = x - mx_ref[at, :]
                ey = y - my_ref[at, :]
                ez = z - mz_ref[at, :]
                fall = jnp.exp2(shift - (ex * ex + ey * ey + ez * ez))
                wk = jnp.exp2(fall) * w
                h = wk * fall * (ma_ref[at, :] * ip + mb_ref[at, :])
                dx = h * ex
                dy = h * ey
                dz = h * ez
                px = px + fold8(dx)
                py = py + fold8(dy)
                pz = pz + fold8(dz)
                ax_ref[at, :] += dx
                ay_ref[at, :] += dy
                az_ref[at, :] += dz
                ad_ref[at, :] += wk * ip
        loss = jnp.where(w > 0.0, kernel_width * sharp - kernel_width * jnp.log(zp), 0.0)
        reply_ref[slot, 0:1, :] = loss
        for f, v in enumerate((px, py, pz)):
            reply_ref[slot, f + 1 : f + 2, :] = jnp.sum(v, axis=0, keepdims=True) * grad_unit
        return carry

    lax.fori_loop(0, used_ref[0], use, 0)

    def sum_row(r, carry):
        for f, ref in enumerate((ax_ref, ay_ref, az_ref, ad_ref)):
            unit = -grad_unit if f < 3 else 1.0
            for c in range(chunks):
                height = min(LANES, width - c * LANES)
                line_ref[f, r, :, c * LANES : (c + 1) * LANES] = (
                    gather_sum(ref, r * width + c * LANES, height) * unit
                )
        return carry

    lax.fori_loop(0, planes * rows, sum_row, 0)
    for f in range(4):
        for p in range(planes):
            for r in range(rows):
                if p == 0:
                    grad_ref[f, r : r + 1, :] = line_ref[f, r]
                else:
                    other_ref[p - 1, f, r : r + 1, :] = line_ref[f, p * rows + r]


def pick_kernel(slot_ref, reply_ref, out_ref):
    def one(b, carry):
        out_ref[b] = reply_ref[slot_ref[b]]
        return carry

    lax.fori_loop(0, out_ref.shape[0], one, 0, unroll=4)


def swap(value, axis, odd):
    count = lax.axis_size(axis)
    pairs = []
    for i in range(odd, count - 1, 2):
        pairs += [(i, i + 1), (i + 1, i)]
    if odd and count % 2 == 0 and count > 2:
        pairs += [(0, count - 1), (count - 1, 0)]
    return lax.ppermute(value, axis, pairs)


def trade(low, high, axis):
    count = lax.axis_size(axis)
    here = lax.axis_index(axis)
    even = here % 2 == 0
    first = swap(jnp.where(even, high, low), axis, 0)
    second = swap(jnp.where(even, low, high), axis, 1) if count > 2 else jnp.zeros_like(first)
    from_low = jnp.where(here > 0, jnp.where(even, second, first), 0.0)
    from_high = jnp.where(here < count - 1, jnp.where(even, first, second), 0.0)
    return from_low, from_high


def step(
    point_xyz, point_weight, block_cell, block_count, gauss_mean, gauss_opacity, gauss_count
):
    blocks, _, pts = point_xyz.shape
    span_x, span_y, span_z, _, slots = gauss_mean.shape
    spans = (span_x, span_y, span_z)
    sizes = tuple(lax.axis_size(a) for a in AXES)
    if span_x != 1 or slots != SLOTS or pts != LANES or span_y < 2 or span_z % 4:
        raise ValueError("unsupported brick")
    bricks = sizes[0] * sizes[1] * sizes[2]
    places = bricks * MOST
    f32 = jnp.float32

    outgoing, send_slot = route(spans, sizes, point_xyz, point_weight, block_cell, block_count)
    incoming = lax.all_to_all(outgoing, AXES, split_axis=0, concat_axis=0, tiled=True)

    present = jnp.arange(slots, dtype=jnp.int32) < gauss_count[..., None]
    own = jnp.concatenate([gauss_mean, jnp.where(present, gauss_opacity, 0.0)[..., None, :]], axis=3)
    own = own[0].transpose(2, 0, 1, 3).reshape(4, 1, span_y, span_z * slots)
    if sizes[0] == 2:
        other = swap(own, "gx", 0)
        stack = jnp.concatenate([own, other], axis=1)
    else:
        stack = jnp.concatenate([own, *trade(own, own, "gx")], axis=1)
    planes = stack.shape[1]
    rows = span_y + 2
    low, high = trade(stack[:, :, :1], stack[:, :, -1:], "gy")
    stack = jnp.concatenate([low, stack, high], axis=2)
    low, high = trade(stack[..., :slots], stack[..., -slots:], "gz")
    width = (span_z + 2) * slots
    wide = -(-width // LANES) * LANES
    stack = jnp.concatenate(
        [low, stack, high, jnp.zeros((4, planes, rows, wide - width), f32)], axis=3
    )

    table = pltpu.VMEM((planes * rows * width, LANES), f32)
    turn = pltpu.VMEM((planes * 3 * 96, LANES), f32)
    feats, points, part, mirror, label, order, used = pl.pallas_call(
        functools.partial(density_kernel, spans, planes),
        out_shape=(
            jax.ShapeDtypeStruct((planes * rows * width, LANES), jnp.bfloat16),
            jax.ShapeDtypeStruct(((places + 8) * 8, LANES), f32),
            jax.ShapeDtypeStruct((planes, rows, wide), f32),
            jax.ShapeDtypeStruct((planes, rows, wide), f32),
            jax.ShapeDtypeStruct((places + 1,), jnp.int32),
            jax.ShapeDtypeStruct((places + 3,), jnp.int32),
            jax.ShapeDtypeStruct((1,), jnp.int32),
        ),
        in_specs=[VMEM, VMEM],
        out_specs=(VMEM, VMEM, VMEM, VMEM, SMEM, SMEM, SMEM),
        scratch_shapes=[
            pltpu.VMEM(((places + 8) * 32, LANES), f32),
            pltpu.VMEM((5, places + 8, LANES), f32),
            pltpu.VMEM((LANES * planes * 8, LANES), f32),
            table,
            table,
            pltpu.VMEM((1, planes * rows, 1, wide), f32),
            turn,
            turn,
        ],
        cost_estimate=pl.CostEstimate(flops=15000000*1000, bytes_accessed=1 << 18, transcendentals=0),
        name="density",
    )(incoming, stack)

    if sizes[0] == 2:
        part = part + swap(mirror, "gx", 0)
    else:
        low, high = trade(part[1], part[2], "gx")
        whole = part[0] + low + high
        part = jnp.stack([whole, *trade(whole, whole, "gx")])
    low, high = trade(part[:, :2], part[:, -2:], "gy")
    part = jnp.concatenate([part[:, :2] + low, part[:, 2:-2], part[:, -2:] + high], axis=1)
    edge = 2 * slots
    low, high = trade(part[..., :edge], part[..., width - edge : width], "gz")
    part = jnp.concatenate(
        [
            part[..., :edge] + low,
            part[..., edge : width - edge],
            part[..., width - edge : width] + high,
            jnp.zeros((planes, rows, wide - width), f32),
        ],
        axis=2,
    )
    reply, grad, other = pl.pallas_call(
        functools.partial(gradient_kernel, spans, planes),
        out_shape=(
            jax.ShapeDtypeStruct((places, 4, LANES), f32),
            jax.ShapeDtypeStruct((4, rows, wide), f32),
            jax.ShapeDtypeStruct((planes - 1, 4, rows, wide), f32),
        ),
        in_specs=[VMEM, VMEM, VMEM, SMEM, SMEM, SMEM],
        out_specs=(VMEM, VMEM, VMEM),
        scratch_shapes=[table] * 9
        + [pltpu.VMEM((4, planes * rows, 1, wide), f32), pltpu.VMEM((2, planes * 3 * 96, LANES), f32)],
        cost_estimate=pl.CostEstimate(flops=28000000*1000, bytes_accessed=1 << 18, transcendentals=0),
        name="gradient",
    )(feats, points.reshape(places + 8, 8, LANES), part, label, order, used)

    answer = lax.all_to_all(reply, AXES, split_axis=0, concat_axis=0, tiled=True)
    point_out = pl.pallas_call(
        pick_kernel,
        out_shape=jax.ShapeDtypeStruct((blocks, 4, pts), f32),
        in_specs=[SMEM, VMEM],
        out_specs=VMEM,
        cost_estimate=pl.CostEstimate(flops=2000000*1000, bytes_accessed=1 << 18, transcendentals=0),
        name="pick",
    )(send_slot, answer)

    if sizes[0] == 2:
        grad = grad + swap(other[0], "gx", 0)
    else:
        low, high = trade(other[0], other[1], "gx")
        grad = grad + low + high
    low, high = trade(grad[:, :1], grad[:, -1:], "gy")
    grad = jnp.concatenate(
        [grad[:, 1:2] + low, grad[:, 2:-2], grad[:, -2:-1] + high], axis=1
    )
    low, high = trade(grad[..., :slots], grad[..., width - slots : width], "gz")
    grad = jnp.concatenate(
        [
            grad[..., slots : 2 * slots] + low,
            grad[..., 2 * slots : width - 2 * slots],
            grad[..., width - 2 * slots : width - slots] + high,
        ],
        axis=2,
    )
    grad = grad.reshape(4, span_y, span_z, slots).transpose(1, 2, 0, 3)[None]
    total_g = 1.0 + part[0, 1:-1, slots : width - slots].reshape(1, span_y, span_z, slots)
    opacity = jnp.where(
        present,
        kernel_width * sharp - kernel_width * jnp.log(total_g) - kernel_width * grad[..., 3, :],
        0.0,
    )
    gauss_grad = jnp.concatenate([grad[..., :3, :], opacity[..., None, :]], axis=3)
    return point_out, gauss_grad


def solution(mesh):
    return jax.shard_map(
        step,
        mesh=mesh,
        in_specs=(
            P(AXES, None, None),
            P(AXES, None),
            P(AXES),
            P(AXES),
            P("gx", "gy", "gz", None, None),
            P("gx", "gy", "gz", None),
            P("gx", "gy", "gz"),
        ),
        out_specs=(P(AXES, None, None), P("gx", "gy", "gz", None, None)),
        check_vma=False,
    )
```

```python
import functools
import math

import jax
import jax.numpy as jnp
from jax import lax
from jax.experimental import pallas as pl
from jax.experimental.pallas import tpu as pltpu
from jax.sharding import PartitionSpec as P


MOST = 2
AXES = ("gx", "gy", "gz")
LANES = 128
SLOTS = 32

kernel_width = 0.05
cutoff_sq = 0.5
sharp = cutoff_sq / kernel_width
log2e = math.log2(math.e)
scale = math.sqrt(log2e / cutoff_sq)
gain = sharp * log2e
shift = math.log2(gain)
grad_unit = 2.0 / (gain * scale)

VMEM = pl.BlockSpec(memory_space=pltpu.VMEM)
SMEM = pl.BlockSpec(memory_space=pltpu.SMEM)


def div_rem(value, size):
    if size & (size - 1) == 0:
        return lax.shift_right_logical(value, size.bit_length() - 1), value & (size - 1)
    return lax.div(value, size), lax.rem(value, size)


def route_kernel(spans, sizes, cell_ref, count_ref, xyz_ref, wt_ref, out_ref, slot_ref, used_ref):
    _, blocks, pts = xyz_ref.shape
    bricks = sizes[0] * sizes[1] * sizes[2]
    lane = lax.broadcasted_iota(jnp.int32, (1, pts), 1)
    out_ref[:, :, : 4 * pts] = jnp.zeros((out_ref.shape[0], 1, 4 * pts), jnp.float32)
    out_ref[:, :, 4 * pts :] = jnp.full((out_ref.shape[0], 1, LANES), -1.0, jnp.float32)

    def clear(i, carry):
        used_ref[i] = 0
        return carry

    lax.fori_loop(0, bricks, clear, 0, unroll=8)

    def one(b, carry):
        rest, along_z = div_rem(cell_ref[b], spans[2] * sizes[2])
        along_x, along_y = div_rem(rest, spans[1] * sizes[1])
        brick_x, in_x = div_rem(along_x, spans[0])
        brick_y, in_y = div_rem(along_y, spans[1])
        brick_z, in_z = div_rem(along_z, spans[2])
        target = (brick_x * sizes[1] + brick_y) * sizes[2] + brick_z
        local = (in_x * spans[1] + in_y) * spans[2] + in_z
        before = used_ref[target]
        used_ref[target] = before + 1
        slot = target * MOST + before
        slot_ref[b] = slot
        count = count_ref[b]
        for f in range(3):
            out_ref[slot, :, f * pts : (f + 1) * pts] = xyz_ref[f, pl.ds(b, 1), :]
        out_ref[slot, :, 3 * pts : 4 * pts] = jnp.where(lane < count, wt_ref[pl.ds(b, 1), :], 0.0)
        out_ref[slot, :, 4 * pts :] = jnp.full((1, LANES), local, jnp.int32).astype(jnp.float32)
        return carry

    lax.fori_loop(0, blocks, one, 0, unroll=4)


def route(spans, sizes, point_xyz, point_weight, block_cell, block_count):
    blocks, _, pts = point_xyz.shape
    bricks = sizes[0] * sizes[1] * sizes[2]
    places = bricks * MOST
    f32 = jnp.float32
    return pl.pallas_call(
        functools.partial(route_kernel, spans, sizes),
        out_shape=(
            jax.ShapeDtypeStruct((places, 1, 5 * pts), f32),
            jax.ShapeDtypeStruct((blocks,), jnp.int32),
        ),
        in_specs=[SMEM, SMEM, VMEM, VMEM],
        out_specs=(VMEM, SMEM),
        scratch_shapes=[pltpu.SMEM((bricks,), jnp.int32)],
        cost_estimate=pl.CostEstimate(flops=3000000*1000, bytes_accessed=1 << 18, transcendentals=0),
        name="route",
    )(block_cell, block_count, point_xyz.transpose(1, 0, 2), point_weight)


def lane_ids(shape):
    return lax.broadcasted_iota(jnp.int32, shape, len(shape) - 1)


def sub_ids(shape):
    return lax.broadcasted_iota(jnp.int32, shape, len(shape) - 2)


def bases_of(label, spans, rows, planes):
    in_y, in_z = div_rem(label, spans[2])
    cells = spans[2] + 2
    return [
        pl.multiple_of(((p * rows + in_y + dy) * cells + in_z) * SLOTS, SLOTS)
        for p in range(planes)
        for dy in range(3)
    ]


def gather_sum(acc_ref, base, height):
    lane = lane_ids((8, LANES))
    sub = sub_ids((8, LANES))
    total = None
    for t in range(height // 8):
        at = pl.ds(pl.multiple_of(base + 8 * t, 8), 8)
        part = jnp.sum(acc_ref[at, :], axis=1, keepdims=True)
        part = jnp.where(lane == sub + 8 * t, part, 0.0)
        total = part if total is None else total + part
    return jnp.sum(total, axis=0, keepdims=True)


def clear(refs):
    step = 96

    def some(i, carry):
        at = pl.ds(pl.multiple_of(i * step, 8), step)
        for ref in refs:
            ref[at, :] = jnp.zeros((step, ref.shape[1]), jnp.float32)
        return carry

    lax.fori_loop(0, refs[0].shape[0] // step, some, 0)


def fold8(value):
    return jnp.sum(value.reshape(value.shape[0] // 8, 8, value.shape[1]), axis=0)


def pieces(value):
    first = value.astype(jnp.bfloat16).astype(jnp.float32)
    rest = value - first
    second = rest.astype(jnp.bfloat16).astype(jnp.float32)
    return first, second, rest - second


def cross_rows(x, y, z, twice):
    rows = []
    split = [pieces(v) for v in (x, y, z)]
    for one in split:
        rows += list(one) if twice else [one[0]] * 3
    for one in split:
        rows += list(one[:2]) if twice else [one[1]] * 2
    for one in split:
        rows += [one[0]] if twice else [one[2]]
    return [v + v for v in rows] if twice else rows


PIECE_ROWS = ((0, 9, 15), (3, 11, 16), (6, 13, 17), (24, 25, 26))


def selector(fields):
    shape = (LANES, LANES * len(fields))
    row = sub_ids(shape)
    lane = lane_ids(shape)
    pick = None
    for n, f in enumerate(fields):
        hit = (row == PIECE_ROWS[f][0]) | (row == PIECE_ROWS[f][1]) | (row == PIECE_ROWS[f][2])
        hit = hit & (lane >= n * LANES) & (lane < (n + 1) * LANES)
        pick = hit if pick is None else pick | hit
    return jnp.where(pick, 1.0, 0.0).astype(jnp.bfloat16)


def product(left, right):
    return jnp.dot(left, right, preferred_element_type=jnp.float32)


def fill(slot, t_ref, label_ref, pair_ref, feat_ref, spans, rows, planes):
    label = label_ref[slot]
    _, in_z = div_rem(label, spans[2])
    near, _ = div_rem(in_z, 4)
    pitch = pair_ref.shape[0] // 24
    part = [pair_ref[pl.ds(8 * t * pitch + slot, 8, stride=pitch), :] for t in range(3)]
    part.append(jnp.zeros((8, LANES), jnp.float32))
    right = jnp.concatenate(part * 4, axis=0)
    right = jnp.where(lax.shift_right_logical(sub_ids(right.shape), 5) == near, right, 0.0)
    right = right.astype(jnp.bfloat16)
    left = [feat_ref[pl.ds(base, 96), :] for base in bases_of(label, spans, rows, planes)]
    t_ref[...] = product(jnp.concatenate(left, axis=0), right)


def in_turn(used, list_ref, ta_ref, tb_ref, load, use):
    load(list_ref[0], ta_ref)

    def two(i, carry):
        first = list_ref[2 * i]
        second = list_ref[2 * i + 1]
        load(second, tb_ref)
        use(first, ta_ref)
        load(list_ref[2 * i + 2], ta_ref)
        use(second, tb_ref)
        return carry

    lax.fori_loop(0, lax.shift_right_logical(used + 1, 1), two, 0)


def density_kernel(
    spans, planes, in_ref, gauss_ref,
    feat_ref, point_ref, zg_ref, zr_ref, label_ref, list_ref, used_ref,
    pair_ref, raw_ref, fs_ref, ma_ref, acc_ref, line_ref, ta_ref, tb_ref,
):
    slots = in_ref.shape[0]
    pts = LANES
    rows = spans[1] + 2
    width = (spans[2] + 2) * SLOTS
    chunks = -(-width // LANES)
    here = [lax.axis_index(a) * s for a, s in zip(AXES, spans)]
    ref_x = here[0].astype(jnp.float32) + 0.5 * spans[0]
    ref_y = here[1].astype(jnp.float32) + 0.5 * spans[1]
    ref_z = here[2].astype(jnp.float32) + 2.0

    for s in range(slots):
        label_ref[s] = in_ref[s, :, 4 * pts :].astype(jnp.int32)[0, 0]
        for f in range(5):
            raw_ref[f, s : s + 1, :] = in_ref[s, :, f * pts : (f + 1) * pts]
    for f in range(5):
        raw_ref[f, slots : slots + 8, :] = jnp.zeros((8, pts), jnp.float32)
    label_ref[slots] = 0

    def order(s, n):
        list_ref[n] = s
        return n + (label_ref[s] >= 0).astype(jnp.int32)

    used = lax.fori_loop(0, slots, order, 0)
    for n in range(3):
        list_ref[used + n] = slots
    used_ref[0] = used

    for g in range(slots // 8 + 1):
        x, y, z, w, lab = (raw_ref[f, 8 * g : 8 * g + 8, :] for f in range(5))
        lab = jnp.maximum(lab, 0.0)
        in_z = lab - jnp.floor((lab + 0.5) * (1.0 / spans[2])) * spans[2]
        near = jnp.floor((in_z + 0.5) * 0.25) * 4.0
        x = (x - ref_x) * scale
        y = (y - ref_y) * scale
        at_z = (z - (ref_z + near)) * scale
        z = (z - ref_z) * scale
        one = jnp.ones_like(x)
        lines = cross_rows(x, y, at_z, True) + [one] * 3
        lines += list(pieces(0.0 - (x * x + y * y + at_z * at_z)))
        for k, v in enumerate(lines):
            top = k * (slots + 8) + 8 * g
            pair_ref[top : top + 8, :] = v
        for f, v in enumerate((x, y, z, w, one, one, one, one)):
            point_ref[pl.ds(g * 64 + f, 8, stride=8), :] = v

    tall = planes * 8
    fs_ref[...] = jnp.zeros(fs_ref.shape, jnp.float32)
    for c in range(chunks):
        height = min(LANES, width - c * LANES)
        lanes = slice(c * LANES, (c + 1) * LANES)
        for p in range(planes):
            x, y, z, a = (gauss_ref[f, p, :, lanes] for f in range(4))
            x = (x - ref_x) * scale
            y = (y - ref_y) * scale
            plane_sq = x * x + y * y
            for q in range(4):
                at_z = (z - (ref_z + 4.0 * q)) * scale
                lines = cross_rows(x, y, at_z, False)
                lines += list(pieces(shift - (plane_sq + at_z * at_z)))
                lines += [jnp.ones_like(x)] * 3
                if q == 0:
                    lines += list(pieces(a))
                for k, v in enumerate(lines):
                    top = (32 * q + k) * tall + 8 * p
                    fs_ref[top : top + rows, :] = v
        for p in range(planes):
            for r in range(rows):
                block = jnp.concatenate(
                    [fs_ref[pl.ds(8 * t * tall + 8 * p + r, 8, stride=tall), :] for t in range(16)], axis=0
                )
                block = block.T.astype(jnp.bfloat16)
                top = (p * rows + r) * width + c * LANES
                feat_ref[top : top + height, :] = block[:height]
    pick = selector((3,))
    for r in range(planes * rows):
        ma_ref[r * width : (r + 1) * width, :] = product(feat_ref[r * width : (r + 1) * width, :], pick)
    clear((acc_ref,))

    def load(slot, t_ref):
        fill(slot, t_ref, label_ref, pair_ref, feat_ref, spans, rows, planes)

    def use(slot, t_ref):
        w = point_ref[pl.ds(pl.multiple_of(slot * 8, 8), 8), :][3:4]
        total = jnp.zeros((8, LANES), jnp.float32)
        for j, base in enumerate(bases_of(label_ref[slot], spans, rows, planes)):
            for c in range(3):
                at = pl.ds(pl.multiple_of(base + c * SLOTS, SLOTS), SLOTS)
                top = j * 96 + c * SLOTS
                kern = jnp.exp2(jnp.exp2(t_ref[top : top + SLOTS, :]))
                total = total + fold8(kern * ma_ref[at, :])
                acc_ref[at, :] += kern * w
        here = pl.ds(pl.multiple_of(slot * 8, 8), 8)
        zp = 1.0 + jnp.sum(total, axis=0, keepdims=True)
        old = point_ref[here, :]
        point_ref[here, :] = jnp.where(sub_ids(old.shape) == 4, zp, old)

    in_turn(used, list_ref, ta_ref, tb_ref, load, use)

    def sum_row(r, carry):
        for c in range(chunks):
            height = min(LANES, width - c * LANES)
            line_ref[0, r, :, c * LANES : (c + 1) * LANES] = gather_sum(
                acc_ref, r * width + c * LANES, height
            )
        return carry

    lax.fori_loop(0, planes * rows, sum_row, 0)
    for p in range(planes):
        for r in range(rows):
            zg_ref[p, r : r + 1, :] = line_ref[0, p * rows + r]
            zr_ref[planes - 1 - p, r : r + 1, :] = line_ref[0, p * rows + r]


def gradient_kernel(
    spans, planes, feat_ref, point_ref, zg_ref, first_ref, second_ref, label_ref, list_ref, used_ref,
    reply_ref, grad_ref, other_ref, whole_ref,
    mx_ref, my_ref, mz_ref, ma_ref, mb_ref, ax_ref, ay_ref, az_ref, ad_ref, line_ref, t_ref,
):
    rows = spans[1] + 2
    width = (spans[2] + 2) * SLOTS
    chunks = -(-width // LANES)
    pick = selector((0, 1, 2, 3))
    for r in range(planes * rows):
        at = slice(r * width, (r + 1) * width)
        both = product(feat_ref[at, :], pick)
        for f, ref in enumerate((mx_ref, my_ref, mz_ref, ma_ref)):
            ref[at, :] = both[:, f * LANES : (f + 1) * LANES]
    tall = planes * 8
    spare = jnp.zeros((LANES - 3 * tall, LANES), jnp.float32)
    here = lax.axis_index("gz")
    odd = (here & 1).astype(jnp.float32)
    lower = jnp.where(here > 0, 1.0, 0.0)
    upper = jnp.where(here < lax.axis_size("gz") - 1, 1.0, 0.0)
    edge = jnp.zeros((rows, LANES - 2 * SLOTS), jnp.float32)
    columns = []
    for c in range(chunks):
        lanes = slice(c * LANES, (c + 1) * LANES)
        block = []
        for p in range(planes):
            total = zg_ref[p, :, lanes]
            from_first = odd if c == 0 else 1.0 - odd
            if c in (0, chunks - 1):
                came = first_ref[p] * from_first + second_ref[p] * (1.0 - from_first)
                came = came * (lower if c == 0 else upper)
                total = total + jnp.concatenate([came, edge], axis=1)
            total = 1.0 + total
            if p == 0:
                whole_ref[:, lanes] = total
            block.append(1.0 / total)
            block.append(jnp.ones((8 - rows, LANES), jnp.float32))
        block = jnp.concatenate(block, axis=0)
        columns.append(jnp.concatenate([*pieces(block), spare], axis=0).T.astype(jnp.bfloat16))
    columns = jnp.concatenate(columns, axis=0)[:width]
    line = sub_ids((LANES, LANES))
    for p in range(planes):
        for r in range(rows):
            n = p * 8 + r
            at = slice((p * rows + r) * width, (p * rows + r + 1) * width)
            hit = (line == n) | (line == n + tall) | (line == n + 2 * tall)
            mb_ref[at, :] = ma_ref[at, :] * product(columns, jnp.where(hit, 1.0, 0.0).astype(jnp.bfloat16))
    clear((ax_ref, ay_ref, az_ref, ad_ref))

    def use(i, carry):
        slot = list_ref[i]
        x, y, z, w, zp = (point_ref[slot, f : f + 1, :] for f in range(5))
        ip = 1.0 / zp
        px = py = pz = jnp.zeros((8, LANES), jnp.float32)
        for base in bases_of(label_ref[slot], spans, rows, planes):
            for c in range(3):
                at = pl.ds(pl.multiple_of(base + c * SLOTS, SLOTS), SLOTS)
                ex = x - mx_ref[at, :]
                ey = y - my_ref[at, :]
                ez = z - mz_ref[at, :]
                fall = jnp.exp2(shift - (ex * ex + ey * ey + ez * ez))
                wk = jnp.exp2(fall) * w
                h = wk * fall * (ma_ref[at, :] * ip + mb_ref[at, :])
                dx = h * ex
                dy = h * ey
                dz = h * ez
                px = px + fold8(dx)
                py = py + fold8(dy)
                pz = pz + fold8(dz)
                ax_ref[at, :] += dx
                ay_ref[at, :] += dy
                az_ref[at, :] += dz
                ad_ref[at, :] += wk * ip
        loss = jnp.where(w > 0.0, kernel_width * sharp - kernel_width * jnp.log(zp), 0.0)
        reply_ref[slot, 0:1, :] = loss
        for f, v in enumerate((px, py, pz)):
            reply_ref[slot, f + 1 : f + 2, :] = jnp.sum(v, axis=0, keepdims=True) * grad_unit
        return carry

    lax.fori_loop(0, used_ref[0], use, 0)

    def sum_row(r, carry):
        for f, ref in enumerate((ax_ref, ay_ref, az_ref, ad_ref)):
            unit = -grad_unit if f < 3 else 1.0
            for c in range(chunks):
                height = min(LANES, width - c * LANES)
                line_ref[f, r, :, c * LANES : (c + 1) * LANES] = (
                    gather_sum(ref, r * width + c * LANES, height) * unit
                )
        return carry

    lax.fori_loop(0, planes * rows, sum_row, 0)
    for f in range(4):
        for p in range(planes):
            for r in range(rows):
                if p == 0:
                    grad_ref[f, r : r + 1, :] = line_ref[f, r]
                else:
                    other_ref[p - 1, f, r : r + 1, :] = line_ref[f, p * rows + r]


def pick_kernel(slot_ref, reply_ref, out_ref):
    def one(b, carry):
        out_ref[b] = reply_ref[slot_ref[b]]
        return carry

    lax.fori_loop(0, out_ref.shape[0], one, 0, unroll=4)


def pick(send_slot, answer):
    return pl.pallas_call(
        pick_kernel,
        out_shape=jax.ShapeDtypeStruct((send_slot.shape[0],) + answer.shape[1:], jnp.float32),
        in_specs=[SMEM, VMEM],
        out_specs=VMEM,
        cost_estimate=pl.CostEstimate(flops=2000000000, bytes_accessed=1 << 18, transcendentals=0),
        name="pick",
    )(send_slot, answer)


def swap(value, axis, odd):
    count = lax.axis_size(axis)
    pairs = []
    for i in range(odd, count - 1, 2):
        pairs += [(i, i + 1), (i + 1, i)]
    if odd and count % 2 == 0 and count > 2:
        pairs += [(0, count - 1), (count - 1, 0)]
    return lax.ppermute(value, axis, pairs)


def trade_raw(low, high, axis):
    even = lax.axis_index(axis) % 2 == 0
    first = swap(jnp.where(even, high, low), axis, 0)
    if lax.axis_size(axis) == 2:
        return first, jnp.zeros_like(first)
    return first, swap(jnp.where(even, low, high), axis, 1)


def trade(low, high, axis):
    count = lax.axis_size(axis)
    here = lax.axis_index(axis)
    even = here % 2 == 0
    first, second = trade_raw(low, high, axis)
    from_low = jnp.where(here > 0, jnp.where(even, second, first), 0.0)
    from_high = jnp.where(here < count - 1, jnp.where(even, first, second), 0.0)
    return from_low, from_high


def step(
    point_xyz, point_weight, block_cell, block_count, gauss_mean, gauss_opacity, gauss_count
):
    _, _, pts = point_xyz.shape
    span_x, span_y, span_z, _, slots = gauss_mean.shape
    spans = (span_x, span_y, span_z)
    sizes = tuple(lax.axis_size(a) for a in AXES)
    if span_x != 1 or slots != SLOTS or pts != LANES or span_y < 2 or span_z % 4:
        raise ValueError("unsupported brick")
    bricks = sizes[0] * sizes[1] * sizes[2]
    places = bricks * MOST
    f32 = jnp.float32

    outgoing, send_slot = route(spans, sizes, point_xyz, point_weight, block_cell, block_count)
    incoming = lax.all_to_all(outgoing, AXES, split_axis=0, concat_axis=0, tiled=True)

    present = jnp.arange(slots, dtype=jnp.int32) < gauss_count[..., None]
    own = jnp.concatenate([gauss_mean, jnp.where(present, gauss_opacity, 0.0)[..., None, :]], axis=3)
    own = own[0].transpose(2, 0, 1, 3).reshape(4, 1, span_y, span_z * slots)
    if sizes[0] == 2:
        other = swap(own, "gx", 0)
        stack = jnp.concatenate([own, other], axis=1)
    else:
        stack = jnp.concatenate([own, *trade(own, own, "gx")], axis=1)
    planes = stack.shape[1]
    rows = span_y + 2
    low, high = trade(stack[:, :, :1], stack[:, :, -1:], "gy")
    stack = jnp.concatenate([low, stack, high], axis=2)
    low, high = trade(stack[..., :slots], stack[..., -slots:], "gz")
    width = (span_z + 2) * slots
    wide = -(-width // LANES) * LANES
    stack = jnp.concatenate(
        [low, stack, high, jnp.zeros((4, planes, rows, wide - width), f32)], axis=3
    )

    table = pltpu.VMEM((planes * rows * width, LANES), f32)
    turn = pltpu.VMEM((planes * 3 * 96, LANES), f32)
    feats, points, part, mirror, label, order, used = pl.pallas_call(
        functools.partial(density_kernel, spans, planes),
        out_shape=(
            jax.ShapeDtypeStruct((planes * rows * width, LANES), jnp.bfloat16),
            jax.ShapeDtypeStruct(((places + 8) * 8, LANES), f32),
            jax.ShapeDtypeStruct((planes, rows, wide), f32),
            jax.ShapeDtypeStruct((planes, rows, wide), f32),
            jax.ShapeDtypeStruct((places + 1,), jnp.int32),
            jax.ShapeDtypeStruct((places + 3,), jnp.int32),
            jax.ShapeDtypeStruct((1,), jnp.int32),
        ),
        in_specs=[VMEM, VMEM],
        out_specs=(VMEM, VMEM, VMEM, VMEM, SMEM, SMEM, SMEM),
        scratch_shapes=[
            pltpu.VMEM((24 * (places + 8), LANES), f32),
            pltpu.VMEM((5, places + 8, LANES), f32),
            pltpu.VMEM((LANES * planes * 8, LANES), f32),
            table,
            table,
            pltpu.VMEM((1, planes * rows, 1, wide), f32),
            turn,
            turn,
        ],
        cost_estimate=pl.CostEstimate(flops=15000000*1000, bytes_accessed=1 << 18, transcendentals=0),
        name="density",
    )(incoming, stack)

    if sizes[0] == 2:
        part = part + swap(mirror, "gx", 0)
    else:
        low, high = trade(part[1], part[2], "gx")
        whole = part[0] + low + high
        part = jnp.stack([whole, *trade(whole, whole, "gx")])
    low, high = trade(part[:, :2], part[:, -2:], "gy")
    part = jnp.concatenate([part[:, :2] + low, part[:, 2:-2], part[:, -2:] + high], axis=1)
    edge = 2 * slots
    first, second = trade_raw(part[..., :edge], part[..., width - edge : width], "gz")

    reply, grad, other, whole = pl.pallas_call(
        functools.partial(gradient_kernel, spans, planes),
        out_shape=(
            jax.ShapeDtypeStruct((places, 4, LANES), f32),
            jax.ShapeDtypeStruct((4, rows, wide), f32),
            jax.ShapeDtypeStruct((planes - 1, 4, rows, wide), f32),
            jax.ShapeDtypeStruct((rows, wide), f32),
        ),
        in_specs=[VMEM, VMEM, VMEM, VMEM, VMEM, SMEM, SMEM, SMEM],
        out_specs=(VMEM, VMEM, VMEM, VMEM),
        scratch_shapes=[table] * 9
        + [pltpu.VMEM((4, planes * rows, 1, wide), f32), pltpu.VMEM((2, planes * 3 * 96, LANES), f32)],
        cost_estimate=pl.CostEstimate(flops=28000000*1000, bytes_accessed=1 << 18, transcendentals=0),
        name="gradient",
    )(feats, points.reshape(places + 8, 8, LANES), part, first, second, label, order, used)

    answer = lax.all_to_all(reply, AXES, split_axis=0, concat_axis=0, tiled=True)
    point_out = pick(send_slot, answer)
    if sizes[0] == 2:
        grad = grad + swap(other[0], "gx", 0)
    else:
        low, high = trade(other[0], other[1], "gx")
        grad = grad + low + high
    low, high = trade(grad[:, :1], grad[:, -1:], "gy")
    grad = jnp.concatenate(
        [grad[:, 1:2] + low, grad[:, 2:-2], grad[:, -2:-1] + high], axis=1
    )
    low, high = trade(grad[..., :slots], grad[..., width - slots : width], "gz")
    grad = jnp.concatenate(
        [
            grad[..., slots : 2 * slots] + low,
            grad[..., 2 * slots : width - 2 * slots],
            grad[..., width - 2 * slots : width - slots] + high,
        ],
        axis=2,
    )
    grad = grad.reshape(4, span_y, span_z, slots).transpose(1, 2, 0, 3)[None]
    total_g = whole[1:-1, slots : width - slots].reshape(1, span_y, span_z, slots)
    opacity = jnp.where(
        present,
        kernel_width * sharp - kernel_width * jnp.log(total_g) - kernel_width * grad[..., 3, :],
        0.0,
    )
    gauss_grad = jnp.concatenate([grad[..., :3, :], opacity[..., None, :]], axis=3)
    return point_out, gauss_grad


def solution(mesh):
    return jax.shard_map(
        step,
        mesh=mesh,
        in_specs=(
            P(AXES, None, None),
            P(AXES, None),
            P(AXES),
            P(AXES),
            P("gx", "gy", "gz", None, None),
            P("gx", "gy", "gz", None),
            P("gx", "gy", "gz"),
        ),
        out_specs=(P(AXES, None, None), P("gx", "gy", "gz", None, None)),
        check_vma=False,
    )
```

```python
import functools
import math

import jax
import jax.numpy as jnp
from jax import lax
from jax.experimental import pallas as pl
from jax.experimental.pallas import tpu as pltpu
from jax.sharding import PartitionSpec as P


MOST = 2
AXES = ("gx", "gy", "gz")
LANES = 128
SLOTS = 32

kernel_width = 0.05
cutoff_sq = 0.5
sharp = cutoff_sq / kernel_width
log2e = math.log2(math.e)
scale = math.sqrt(log2e / cutoff_sq)
gain = sharp * log2e
shift = math.log2(gain)
grad_unit = 2.0 / (gain * scale)

VMEM = pl.BlockSpec(memory_space=pltpu.VMEM)
SMEM = pl.BlockSpec(memory_space=pltpu.SMEM)


def div_rem(value, size):
    if size & (size - 1) == 0:
        return lax.shift_right_logical(value, size.bit_length() - 1), value & (size - 1)
    return lax.div(value, size), lax.rem(value, size)


def route_kernel(spans, sizes, cell_ref, count_ref, xyz_ref, wt_ref, out_ref, slot_ref, used_ref):
    _, blocks, pts = xyz_ref.shape
    bricks = sizes[0] * sizes[1] * sizes[2]
    lane = lax.broadcasted_iota(jnp.int32, (1, pts), 1)
    out_ref[:, :, : 4 * pts] = jnp.zeros((out_ref.shape[0], 1, 4 * pts), jnp.float32)
    out_ref[:, :, 4 * pts :] = jnp.full((out_ref.shape[0], 1, LANES), -1.0, jnp.float32)

    def clear(i, carry):
        used_ref[i] = 0
        return carry

    lax.fori_loop(0, bricks, clear, 0, unroll=8)

    def one(b, carry):
        rest, along_z = div_rem(cell_ref[b], spans[2] * sizes[2])
        along_x, along_y = div_rem(rest, spans[1] * sizes[1])
        brick_x, in_x = div_rem(along_x, spans[0])
        brick_y, in_y = div_rem(along_y, spans[1])
        brick_z, in_z = div_rem(along_z, spans[2])
        target = (brick_x * sizes[1] + brick_y) * sizes[2] + brick_z
        local = (in_x * spans[1] + in_y) * spans[2] + in_z
        before = used_ref[target]
        used_ref[target] = before + 1
        slot = target * MOST + before
        slot_ref[b] = slot
        count = count_ref[b]
        for f in range(3):
            out_ref[slot, :, f * pts : (f + 1) * pts] = xyz_ref[f, pl.ds(b, 1), :]
        out_ref[slot, :, 3 * pts : 4 * pts] = jnp.where(lane < count, wt_ref[pl.ds(b, 1), :], 0.0)
        out_ref[slot, :, 4 * pts :] = jnp.full((1, LANES), local, jnp.int32).astype(jnp.float32)
        return carry

    lax.fori_loop(0, blocks, one, 0, unroll=4)


def route(spans, sizes, point_xyz, point_weight, block_cell, block_count):
    blocks, _, pts = point_xyz.shape
    bricks = sizes[0] * sizes[1] * sizes[2]
    places = bricks * MOST
    f32 = jnp.float32
    return pl.pallas_call(
        functools.partial(route_kernel, spans, sizes),
        out_shape=(
            jax.ShapeDtypeStruct((places, 1, 5 * pts), f32),
            jax.ShapeDtypeStruct((blocks,), jnp.int32),
        ),
        in_specs=[SMEM, SMEM, VMEM, VMEM],
        out_specs=(VMEM, SMEM),
        scratch_shapes=[pltpu.SMEM((bricks,), jnp.int32)],
        cost_estimate=pl.CostEstimate(flops=3000000*1000, bytes_accessed=1 << 18, transcendentals=0),
        name="route",
    )(block_cell, block_count, point_xyz.transpose(1, 0, 2), point_weight)


def lane_ids(shape):
    return lax.broadcasted_iota(jnp.int32, shape, len(shape) - 1)


def sub_ids(shape):
    return lax.broadcasted_iota(jnp.int32, shape, len(shape) - 2)


def bases_of(label, spans, rows, planes):
    in_y, in_z = div_rem(label, spans[2])
    cells = spans[2] + 2
    return [
        pl.multiple_of(((p * rows + in_y + dy) * cells + in_z) * SLOTS, SLOTS)
        for p in range(planes)
        for dy in range(3)
    ]


def gather_sum(acc_ref, base, height):
    lane = lane_ids((8, LANES))
    sub = sub_ids((8, LANES))
    total = None
    for t in range(height // 8):
        at = pl.ds(pl.multiple_of(base + 8 * t, 8), 8)
        part = jnp.sum(acc_ref[at, :], axis=1, keepdims=True)
        part = jnp.where(lane == sub + 8 * t, part, 0.0)
        total = part if total is None else total + part
    return jnp.sum(total, axis=0, keepdims=True)


def clear(refs):
    step = 96

    def some(i, carry):
        at = pl.ds(pl.multiple_of(i * step, 8), step)
        for ref in refs:
            ref[at, :] = jnp.zeros((step, ref.shape[1]), jnp.float32)
        return carry

    lax.fori_loop(0, refs[0].shape[0] // step, some, 0)


def fold8(value):
    return jnp.sum(value.reshape(value.shape[0] // 8, 8, value.shape[1]), axis=0)


def pieces(value):
    first = value.astype(jnp.bfloat16).astype(jnp.float32)
    rest = value - first
    second = rest.astype(jnp.bfloat16).astype(jnp.float32)
    return first, second, rest - second


def cross_rows(x, y, z, twice):
    rows = []
    split = [pieces(v) for v in (x, y, z)]
    for one in split:
        rows += list(one) if twice else [one[0]] * 3
    for one in split:
        rows += list(one[:2]) if twice else [one[1]] * 2
    for one in split:
        rows += [one[0]] if twice else [one[2]]
    return [v + v for v in rows] if twice else rows


PIECE_ROWS = ((0, 9, 15), (3, 11, 16), (6, 13, 17), (24, 25, 26))


def selector(fields):
    shape = (LANES, LANES * len(fields))
    row = sub_ids(shape)
    lane = lane_ids(shape)
    pick = None
    for n, f in enumerate(fields):
        hit = (row == PIECE_ROWS[f][0]) | (row == PIECE_ROWS[f][1]) | (row == PIECE_ROWS[f][2])
        hit = hit & (lane >= n * LANES) & (lane < (n + 1) * LANES)
        pick = hit if pick is None else pick | hit
    return jnp.where(pick, 1.0, 0.0).astype(jnp.bfloat16)


def product(left, right):
    return jnp.dot(left, right, preferred_element_type=jnp.float32)


def fill(slot, t_ref, label_ref, pair_ref, feat_ref, spans, rows, planes):
    label = label_ref[slot]
    _, in_z = div_rem(label, spans[2])
    near, _ = div_rem(in_z, 4)
    pitch = pair_ref.shape[0] // 24
    part = [pair_ref[pl.ds(8 * t * pitch + slot, 8, stride=pitch), :] for t in range(3)]
    part.append(jnp.zeros((8, LANES), jnp.float32))
    right = jnp.concatenate(part * 4, axis=0)
    right = jnp.where(lax.shift_right_logical(sub_ids(right.shape), 5) == near, right, 0.0)
    right = right.astype(jnp.bfloat16)
    left = [feat_ref[pl.ds(base, 96), :] for base in bases_of(label, spans, rows, planes)]
    t_ref[...] = product(jnp.concatenate(left, axis=0), right)


def in_turn(used, list_ref, ta_ref, tb_ref, load, use):
    load(list_ref[0], ta_ref)

    def four(i, carry):
        turn = [list_ref[4 * i + n] for n in range(5)]
        tables = (ta_ref, tb_ref)
        for n in range(4):
            load(turn[n + 1], tables[(n + 1) % 2])
            use(turn[n], tables[n % 2])
        return carry

    lax.fori_loop(0, lax.shift_right_logical(used + 3, 2), four, 0)


def density_kernel(
    spans, planes, in_ref, gauss_ref,
    feat_ref, point_ref, zg_ref, zr_ref, label_ref, list_ref, used_ref,
    pair_ref, raw_ref, fs_ref, ma_ref, acc_ref, line_ref, ta_ref, tb_ref,
):
    slots = in_ref.shape[0]
    pts = LANES
    rows = spans[1] + 2
    width = (spans[2] + 2) * SLOTS
    chunks = -(-width // LANES)
    here = [lax.axis_index(a) * s for a, s in zip(AXES, spans)]
    ref_x = here[0].astype(jnp.float32) + 0.5 * spans[0]
    ref_y = here[1].astype(jnp.float32) + 0.5 * spans[1]
    ref_z = here[2].astype(jnp.float32) + 2.0

    for s in range(slots):
        label_ref[s] = in_ref[s, :, 4 * pts :].astype(jnp.int32)[0, 0]
        for f in range(5):
            raw_ref[f, s : s + 1, :] = in_ref[s, :, f * pts : (f + 1) * pts]
    for f in range(5):
        raw_ref[f, slots : slots + 8, :] = jnp.zeros((8, pts), jnp.float32)
    label_ref[slots] = 0

    def order(s, n):
        list_ref[n] = s
        return n + (label_ref[s] >= 0).astype(jnp.int32)

    used = lax.fori_loop(0, slots, order, 0)
    for n in range(5):
        list_ref[used + n] = slots
    used_ref[0] = used

    for g in range(slots // 8 + 1):
        x, y, z, w, lab = (raw_ref[f, 8 * g : 8 * g + 8, :] for f in range(5))
        lab = jnp.maximum(lab, 0.0)
        in_z = lab - jnp.floor((lab + 0.5) * (1.0 / spans[2])) * spans[2]
        near = jnp.floor((in_z + 0.5) * 0.25) * 4.0
        x = (x - ref_x) * scale
        y = (y - ref_y) * scale
        at_z = (z - (ref_z + near)) * scale
        z = (z - ref_z) * scale
        one = jnp.ones_like(x)
        lines = cross_rows(x, y, at_z, True) + [one] * 3
        lines += list(pieces(0.0 - (x * x + y * y + at_z * at_z)))
        for k, v in enumerate(lines):
            top = k * (slots + 8) + 8 * g
            pair_ref[top : top + 8, :] = v
        for f, v in enumerate((x, y, z, w, one, one, one, one)):
            point_ref[pl.ds(g * 64 + f, 8, stride=8), :] = v

    tall = planes * 8
    fs_ref[...] = jnp.zeros(fs_ref.shape, jnp.float32)
    for c in range(chunks):
        height = min(LANES, width - c * LANES)
        lanes = slice(c * LANES, (c + 1) * LANES)
        for p in range(planes):
            x, y, z, a = (gauss_ref[f, p, :, lanes] for f in range(4))
            x = (x - ref_x) * scale
            y = (y - ref_y) * scale
            plane_sq = x * x + y * y
            for q in range(4):
                at_z = (z - (ref_z + 4.0 * q)) * scale
                lines = cross_rows(x, y, at_z, False)
                lines += list(pieces(shift - (plane_sq + at_z * at_z)))
                lines += [jnp.ones_like(x)] * 3
                if q == 0:
                    lines += list(pieces(a))
                for k, v in enumerate(lines):
                    top = (32 * q + k) * tall + 8 * p
                    fs_ref[top : top + rows, :] = v
        for p in range(planes):
            for r in range(rows):
                block = jnp.concatenate(
                    [fs_ref[pl.ds(8 * t * tall + 8 * p + r, 8, stride=tall), :] for t in range(16)], axis=0
                )
                block = block.T.astype(jnp.bfloat16)
                top = (p * rows + r) * width + c * LANES
                feat_ref[top : top + height, :] = block[:height]
    pick = selector((3,))
    for r in range(planes * rows):
        ma_ref[r * width : (r + 1) * width, :] = product(feat_ref[r * width : (r + 1) * width, :], pick)
    clear((acc_ref,))

    def load(slot, t_ref):
        fill(slot, t_ref, label_ref, pair_ref, feat_ref, spans, rows, planes)

    def use(slot, t_ref):
        w = point_ref[pl.ds(pl.multiple_of(slot * 8, 8), 8), :][3:4]
        total = jnp.zeros((8, LANES), jnp.float32)
        for j, base in enumerate(bases_of(label_ref[slot], spans, rows, planes)):
            for c in range(3):
                at = pl.ds(pl.multiple_of(base + c * SLOTS, SLOTS), SLOTS)
                top = j * 96 + c * SLOTS
                kern = jnp.exp2(jnp.exp2(t_ref[top : top + SLOTS, :]))
                total = total + fold8(kern * ma_ref[at, :])
                acc_ref[at, :] += kern * w
        here = pl.ds(pl.multiple_of(slot * 8, 8), 8)
        zp = 1.0 + jnp.sum(total, axis=0, keepdims=True)
        old = point_ref[here, :]
        point_ref[here, :] = jnp.where(sub_ids(old.shape) == 4, zp, old)

    in_turn(used, list_ref, ta_ref, tb_ref, load, use)

    def sum_row(r, carry):
        for c in range(chunks):
            height = min(LANES, width - c * LANES)
            line_ref[0, r, :, c * LANES : (c + 1) * LANES] = gather_sum(
                acc_ref, r * width + c * LANES, height
            )
        return carry

    lax.fori_loop(0, planes * rows, sum_row, 0)
    for p in range(planes):
        for r in range(rows):
            zg_ref[p, r : r + 1, :] = line_ref[0, p * rows + r]
            zr_ref[planes - 1 - p, r : r + 1, :] = line_ref[0, p * rows + r]


def gradient_kernel(
    spans, planes, feat_ref, point_ref, zg_ref, first_ref, second_ref, label_ref, list_ref, used_ref,
    reply_ref, grad_ref, other_ref, whole_ref,
    mx_ref, my_ref, mz_ref, ma_ref, mb_ref, ax_ref, ay_ref, az_ref, ad_ref, line_ref, t_ref,
):
    rows = spans[1] + 2
    width = (spans[2] + 2) * SLOTS
    chunks = -(-width // LANES)
    pick = selector((0, 1, 2, 3))
    for r in range(planes * rows):
        at = slice(r * width, (r + 1) * width)
        both = product(feat_ref[at, :], pick)
        for f, ref in enumerate((mx_ref, my_ref, mz_ref, ma_ref)):
            ref[at, :] = both[:, f * LANES : (f + 1) * LANES]
    tall = planes * 8
    spare = jnp.zeros((LANES - 3 * tall, LANES), jnp.float32)
    here = lax.axis_index("gz")
    odd = (here & 1).astype(jnp.float32)
    lower = jnp.where(here > 0, 1.0, 0.0)
    upper = jnp.where(here < lax.axis_size("gz") - 1, 1.0, 0.0)
    edge = jnp.zeros((rows, LANES - 2 * SLOTS), jnp.float32)
    columns = []
    for c in range(chunks):
        lanes = slice(c * LANES, (c + 1) * LANES)
        block = []
        for p in range(planes):
            total = zg_ref[p, :, lanes]
            from_first = odd if c == 0 else 1.0 - odd
            if c in (0, chunks - 1):
                came = first_ref[p] * from_first + second_ref[p] * (1.0 - from_first)
                came = came * (lower if c == 0 else upper)
                total = total + jnp.concatenate([came, edge], axis=1)
            total = 1.0 + total
            if p == 0:
                whole_ref[:, lanes] = total
            block.append(1.0 / total)
            block.append(jnp.ones((8 - rows, LANES), jnp.float32))
        block = jnp.concatenate(block, axis=0)
        columns.append(jnp.concatenate([*pieces(block), spare], axis=0).T.astype(jnp.bfloat16))
    columns = jnp.concatenate(columns, axis=0)[:width]
    line = sub_ids((LANES, LANES))
    for p in range(planes):
        for r in range(rows):
            n = p * 8 + r
            at = slice((p * rows + r) * width, (p * rows + r + 1) * width)
            hit = (line == n) | (line == n + tall) | (line == n + 2 * tall)
            mb_ref[at, :] = ma_ref[at, :] * product(columns, jnp.where(hit, 1.0, 0.0).astype(jnp.bfloat16))
            for ref in (ax_ref, ay_ref, az_ref, ad_ref):
                ref[at, :] = jnp.zeros((width, LANES), jnp.float32)

    def use(i, carry):
        slot = list_ref[i]
        x, y, z, w, zp = (point_ref[slot, f : f + 1, :] for f in range(5))
        ip = 1.0 / zp
        px = py = pz = jnp.zeros((8, LANES), jnp.float32)
        for base in bases_of(label_ref[slot], spans, rows, planes):
            for c in range(3):
                at = pl.ds(pl.multiple_of(base + c * SLOTS, SLOTS), SLOTS)
                ex = x - mx_ref[at, :]
                ey = y - my_ref[at, :]
                ez = z - mz_ref[at, :]
                fall = jnp.exp2(shift - (ex * ex + ey * ey + ez * ez))
                wk = jnp.exp2(fall) * w
                h = wk * fall * (ma_ref[at, :] * ip + mb_ref[at, :])
                dx = h * ex
                dy = h * ey
                dz = h * ez
                px = px + fold8(dx)
                py = py + fold8(dy)
                pz = pz + fold8(dz)
                ax_ref[at, :] += dx
                ay_ref[at, :] += dy
                az_ref[at, :] += dz
                ad_ref[at, :] += wk * ip
        loss = jnp.where(w > 0.0, kernel_width * sharp - kernel_width * jnp.log(zp), 0.0)
        reply_ref[slot, 0:1, :] = loss
        for f, v in enumerate((px, py, pz)):
            reply_ref[slot, f + 1 : f + 2, :] = jnp.sum(v, axis=0, keepdims=True) * grad_unit
        return carry

    lax.fori_loop(0, used_ref[0], use, 0)

    def sum_row(r, carry):
        for f, ref in enumerate((ax_ref, ay_ref, az_ref, ad_ref)):
            unit = -grad_unit if f < 3 else 1.0
            for c in range(chunks):
                height = min(LANES, width - c * LANES)
                line_ref[f, r, :, c * LANES : (c + 1) * LANES] = (
                    gather_sum(ref, r * width + c * LANES, height) * unit
                )
        return carry

    lax.fori_loop(0, planes * rows, sum_row, 0)
    for f in range(4):
        for p in range(planes):
            for r in range(rows):
                if p == 0:
                    grad_ref[f, r : r + 1, :] = line_ref[f, r]
                else:
                    other_ref[p - 1, f, r : r + 1, :] = line_ref[f, p * rows + r]


def pick_kernel(slot_ref, reply_ref, out_ref):
    def one(b, carry):
        out_ref[b] = reply_ref[slot_ref[b]]
        return carry

    lax.fori_loop(0, out_ref.shape[0], one, 0, unroll=4)


def pick(send_slot, answer):
    return pl.pallas_call(
        pick_kernel,
        out_shape=jax.ShapeDtypeStruct((send_slot.shape[0],) + answer.shape[1:], jnp.float32),
        in_specs=[SMEM, VMEM],
        out_specs=VMEM,
        cost_estimate=pl.CostEstimate(flops=2000000000, bytes_accessed=1 << 18, transcendentals=0),
        name="pick",
    )(send_slot, answer)


def swap(value, axis, odd):
    count = lax.axis_size(axis)
    pairs = []
    for i in range(odd, count - 1, 2):
        pairs += [(i, i + 1), (i + 1, i)]
    if odd and count % 2 == 0 and count > 2:
        pairs += [(0, count - 1), (count - 1, 0)]
    return lax.ppermute(value, axis, pairs)


def trade_raw(low, high, axis):
    even = lax.axis_index(axis) % 2 == 0
    first = swap(jnp.where(even, high, low), axis, 0)
    if lax.axis_size(axis) == 2:
        return first, jnp.zeros_like(first)
    return first, swap(jnp.where(even, low, high), axis, 1)


def trade(low, high, axis):
    count = lax.axis_size(axis)
    here = lax.axis_index(axis)
    even = here % 2 == 0
    first, second = trade_raw(low, high, axis)
    from_low = jnp.where(here > 0, jnp.where(even, second, first), 0.0)
    from_high = jnp.where(here < count - 1, jnp.where(even, first, second), 0.0)
    return from_low, from_high


def step(
    point_xyz, point_weight, block_cell, block_count, gauss_mean, gauss_opacity, gauss_count
):
    _, _, pts = point_xyz.shape
    span_x, span_y, span_z, _, slots = gauss_mean.shape
    spans = (span_x, span_y, span_z)
    sizes = tuple(lax.axis_size(a) for a in AXES)
    if span_x != 1 or slots != SLOTS or pts != LANES or span_y < 2 or span_z % 4:
        raise ValueError("unsupported brick")
    bricks = sizes[0] * sizes[1] * sizes[2]
    places = bricks * MOST
    f32 = jnp.float32

    outgoing, send_slot = route(spans, sizes, point_xyz, point_weight, block_cell, block_count)
    incoming = lax.all_to_all(outgoing, AXES, split_axis=0, concat_axis=0, tiled=True)

    present = jnp.arange(slots, dtype=jnp.int32) < gauss_count[..., None]
    own = jnp.concatenate([gauss_mean, jnp.where(present, gauss_opacity, 0.0)[..., None, :]], axis=3)
    own = own[0].transpose(2, 0, 1, 3).reshape(4, 1, span_y, span_z * slots)
    if sizes[0] == 2:
        other = swap(own, "gx", 0)
        stack = jnp.concatenate([own, other], axis=1)
    else:
        stack = jnp.concatenate([own, *trade(own, own, "gx")], axis=1)
    planes = stack.shape[1]
    rows = span_y + 2
    low, high = trade(stack[:, :, :1], stack[:, :, -1:], "gy")
    stack = jnp.concatenate([low, stack, high], axis=2)
    low, high = trade(stack[..., :slots], stack[..., -slots:], "gz")
    width = (span_z + 2) * slots
    wide = -(-width // LANES) * LANES
    stack = jnp.concatenate(
        [low, stack, high, jnp.zeros((4, planes, rows, wide - width), f32)], axis=3
    )

    table = pltpu.VMEM((planes * rows * width, LANES), f32)
    turn = pltpu.VMEM((planes * 3 * 96, LANES), f32)
    feats, points, part, mirror, label, order, used = pl.pallas_call(
        functools.partial(density_kernel, spans, planes),
        out_shape=(
            jax.ShapeDtypeStruct((planes * rows * width, LANES), jnp.bfloat16),
            jax.ShapeDtypeStruct(((places + 8) * 8, LANES), f32),
            jax.ShapeDtypeStruct((planes, rows, wide), f32),
            jax.ShapeDtypeStruct((planes, rows, wide), f32),
            jax.ShapeDtypeStruct((places + 1,), jnp.int32),
            jax.ShapeDtypeStruct((places + 5,), jnp.int32),
            jax.ShapeDtypeStruct((1,), jnp.int32),
        ),
        in_specs=[VMEM, VMEM],
        out_specs=(VMEM, VMEM, VMEM, VMEM, SMEM, SMEM, SMEM),
        scratch_shapes=[
            pltpu.VMEM((24 * (places + 8), LANES), f32),
            pltpu.VMEM((5, places + 8, LANES), f32),
            pltpu.VMEM((LANES * planes * 8, LANES), f32),
            table,
            table,
            pltpu.VMEM((1, planes * rows, 1, wide), f32),
            turn,
            turn,
        ],
        cost_estimate=pl.CostEstimate(flops=15000000*1000, bytes_accessed=1 << 18, transcendentals=0),
        name="density",
    )(incoming, stack)

    if sizes[0] == 2:
        part = part + swap(mirror, "gx", 0)
    else:
        low, high = trade(part[1], part[2], "gx")
        whole = part[0] + low + high
        part = jnp.stack([whole, *trade(whole, whole, "gx")])
    low, high = trade(part[:, :2], part[:, -2:], "gy")
    part = jnp.concatenate([part[:, :2] + low, part[:, 2:-2], part[:, -2:] + high], axis=1)
    edge = 2 * slots
    first, second = trade_raw(part[..., :edge], part[..., width - edge : width], "gz")

    reply, grad, other, whole = pl.pallas_call(
        functools.partial(gradient_kernel, spans, planes),
        out_shape=(
            jax.ShapeDtypeStruct((places, 4, LANES), f32),
            jax.ShapeDtypeStruct((4, rows, wide), f32),
            jax.ShapeDtypeStruct((planes - 1, 4, rows, wide), f32),
            jax.ShapeDtypeStruct((rows, wide), f32),
        ),
        in_specs=[VMEM, VMEM, VMEM, VMEM, VMEM, SMEM, SMEM, SMEM],
        out_specs=(VMEM, VMEM, VMEM, VMEM),
        scratch_shapes=[table] * 9
        + [pltpu.VMEM((4, planes * rows, 1, wide), f32), pltpu.VMEM((2, planes * 3 * 96, LANES), f32)],
        cost_estimate=pl.CostEstimate(flops=28000000*1000, bytes_accessed=1 << 18, transcendentals=0),
        name="gradient",
    )(feats, points.reshape(places + 8, 8, LANES), part, first, second, label, order, used)

    answer = lax.all_to_all(reply, AXES, split_axis=0, concat_axis=0, tiled=True)
    point_out = pick(send_slot, answer)
    if sizes[0] == 2:
        grad = grad + swap(other[0], "gx", 0)
    else:
        low, high = trade(other[0], other[1], "gx")
        grad = grad + low + high
    low, high = trade(grad[:, :1], grad[:, -1:], "gy")
    grad = jnp.concatenate(
        [grad[:, 1:2] + low, grad[:, 2:-2], grad[:, -2:-1] + high], axis=1
    )
    low, high = trade(grad[..., :slots], grad[..., width - slots : width], "gz")
    grad = jnp.concatenate(
        [
            grad[..., slots : 2 * slots] + low,
            grad[..., 2 * slots : width - 2 * slots],
            grad[..., width - 2 * slots : width - slots] + high,
        ],
        axis=2,
    )
    grad = grad.reshape(4, span_y, span_z, slots).transpose(1, 2, 0, 3)[None]
    total_g = whole[1:-1, slots : width - slots].reshape(1, span_y, span_z, slots)
    opacity = jnp.where(
        present,
        kernel_width * sharp - kernel_width * jnp.log(total_g) - kernel_width * grad[..., 3, :],
        0.0,
    )
    gauss_grad = jnp.concatenate([grad[..., :3, :], opacity[..., None, :]], axis=3)
    return point_out, gauss_grad


def solution(mesh):
    return jax.shard_map(
        step,
        mesh=mesh,
        in_specs=(
            P(AXES, None, None),
            P(AXES, None),
            P(AXES),
            P(AXES),
            P("gx", "gy", "gz", None, None),
            P("gx", "gy", "gz", None),
            P("gx", "gy", "gz"),
        ),
        out_specs=(P(AXES, None, None), P("gx", "gy", "gz", None, None)),
        check_vma=False,
    )
```
